128 devices in a mesh: seq: 32 (over z, x, core), head: 4 (over y).
Axes of the slice: x: 4, y: 4, z: 4, core: 2. Of those that a mesh axis runs over, the one named last changes fastest.
Arguments:
- queries: bfloat16 [32768, 4096], P('seq', 'head'), may hold values from -8 to 8
- key_rows: bfloat16 [32768, 4096], P('seq', 'head'), may hold values from -8 to 8
- value_rows: bfloat16 [32768, 4096], P('seq', 'head'), may hold values from -6 to 6
- random_owner: int32 [512, 3], P('seq'), may hold values from 0 to 31, all different within a row; in each aligned block of 16 rows (0 to 15, 16 to 31, ...) at most 2 rows name the same one
- random_local: int32 [512, 3], P('seq'), may hold values from 0 to 15
- output_weight: bfloat16 [4096, 4096], P('head'), may hold values from -0.09375 to 0.09375
Outputs:
- layer_output: bfloat16 [32768, 4096], P(('seq', 'head'))
The draws below stay inside these ranges and needn't reach their ends.
Inputs may be any that keep to these rules, and one draw needn't show every extreme that they name: `random_owner`: each row names 3 different owners. Among the rows of one device (16 aligned rows) no owner is named more than 2 times, and in some device's rows one owner is named exactly 2 times.
All inputs are finite; a program needn't handle non-finite values.
Results may differ from the reference program's by a relative error of at most 0.0052.
Values may be sent and summed in bfloat16 or wider, within the bound.
A program may use at most 192 MiB of HBM per device.

```python
import math
import jax
import jax.numpy as jnp
import numpy as np
from jax import lax

D = 4096
HEADS = 32
HEAD_DIM = 128
BLOCK = 64
RANDOM = 3
GLOBAL = 128
NB_DEV = 16
CAP = 2
NBLK = 512
TOKENS = 32768
N_SEQ = 32


def query_key_pair(key):
    folded = jax.random.fold_in(key, 11)
    streams = jax.random.split(folded, 8)
    total_width = HEADS * HEAD_DIM
    row_ids = jnp.arange(TOKENS, dtype=jnp.int32)[:, None]
    query_scale = jnp.where(row_ids < GLOBAL, 3.0, 2.0)
    query_values = jax.random.normal(streams[0], (TOKENS, total_width), jnp.float32) * query_scale
    key_values = jax.random.normal(streams[1], (TOKENS, total_width), jnp.float32)
    return (jnp.clip(query_values, -8.0, 8.0), jnp.clip(key_values, -8.0, 8.0))


def draw_queries(key, part):
    return query_key_pair(key)[0].astype(jnp.bfloat16)


def draw_key_rows(key, part):
    return query_key_pair(key)[1].astype(jnp.bfloat16)


def with_ends(values, key, low, largest):
    longest = values.shape.index(max(values.shape))
    spots = []
    for shift in (0, 1):
        where = [jax.random.randint(jax.random.fold_in(key, axis), (), 0, length) for axis, length in enumerate(values.shape)]
        where[longest] = (where[longest] + shift) % values.shape[longest]
        spots.append(tuple(where))
    return values.at[spots[0]].set(low).at[spots[1]].set(largest)


def level_of(stream_key, extent, cuts, low, high):
    gain = 1.0
    for dim, shards_of in cuts:
        steps = jax.random.uniform(jax.random.fold_in(jax.random.fold_in(stream_key, 6), dim), (shards_of,), jnp.float32, low / len(cuts), high / len(cuts))
        gain = gain * jnp.repeat(jnp.exp(steps), extent[dim] // shards_of).reshape((-1,) + (1,) * (len(extent) - 1 - dim))
    return gain


def assign_block(rng, own, number, rows, amount, top, most, slope):
    order = jax.random.permutation(rng, amount)
    crowded, common = shares(amount, rows * top, most, slope, True), shares(amount, rows * top, most, slope, False)
    places = jnp.arange(amount)

    def named(tallies, turn):
        used = int((tallies > 0).sum())
        fixed = max(1, used // 4)
        passed = fixed + (places - fixed + turn * (used - fixed)) % max(1, amount - fixed)
        return jnp.zeros((amount,), jnp.int32).at[order[jnp.where(places < fixed, places, passed)]].set(jnp.asarray(tallies, jnp.int32))

    tallies = jnp.where(number % 4 == 0, named(crowded, number // 4), named(common, number - number // 4 - 1))
    mixed = jax.random.permutation(jax.random.fold_in(own, 3), amount)
    giver, taker = mixed[0:amount // 2 * 2:2], mixed[1:amount // 2 * 2:2]
    margin = jnp.minimum(tallies[giver] - 1, most - tallies[taker]) // 2
    margin = jnp.where((giver == order[0]) | (taker == order[0]) | (tallies[taker] == 0), 0, jnp.maximum(margin, 0))
    passed = jax.random.randint(jax.random.fold_in(own, 4), (amount // 2,), 0, 1 << 20) % (margin + 1)
    tallies = tallies.at[giver].add(-passed).at[taker].add(passed)
    labels = jnp.searchsorted(jnp.cumsum(tallies), jnp.arange(rows * top), side="right").astype(jnp.int32)
    listing = labels.reshape(top, rows).T
    listing = listing[jax.random.permutation(jax.random.fold_in(own, 1), rows)]
    turn = jax.random.randint(jax.random.fold_in(own, 2), (rows, 1), 0, top)
    return jnp.take_along_axis(listing, (jnp.arange(top)[None, :] + turn) % top, axis=1)


def shares(number_of, total, bound, slope, full):
    weights = [(1 << 20) // math.isqrt(grade ** slope) + 1 for grade in range(1, number_of + 1)]
    largest = bound if full else min(bound, max(-(-total // number_of), total * weights[0] // sum(weights)))
    least = 1 if total - largest >= number_of - 1 else 0
    counts, surplus = [largest] + [least] * (number_of - 1), total - largest - least * (number_of - 1)
    while surplus > 0:
        movable = [i for i in range(1, number_of) if counts[i] < largest] or [i for i in range(1, number_of) if counts[i] < bound]
        mass, budget = sum([weights[i] for i in movable]), surplus
        for i in movable:
            extra = min(bound - counts[i], max(1, budget * weights[i] // mass), surplus)
            counts[i] = counts[i] + extra
            surplus = surplus - extra
    return np.array(counts)


def noise(own_key, dims, spread, limit, cuts=(), kind=jnp.bfloat16):
    level = level_of(own_key, dims, cuts, -0.22, 0.18) if cuts else 1.0
    values = jax.random.normal(own_key, dims, jnp.float32) * spread * level
    return jnp.minimum(jnp.maximum(values, -limit), limit).astype(kind)


def setup_inputs(seed: int = 0) -> dict:
    arg_keys = jax.random.split(jax.random.key(seed), 7)
    queries = draw_queries(jax.random.fold_in(arg_keys[6], 71), 0)
    key_rows = draw_key_rows(jax.random.fold_in(arg_keys[6], 71), 0)
    value_rows = noise(arg_keys[2], (TOKENS, HEADS * HEAD_DIM), 1.0, 6.0, ((0, 32), (1, 4)))
    random_owner_keys = jax.random.split(jax.random.fold_in(arg_keys[3], 1), NBLK // NB_DEV)
    random_owner_turns = jax.random.permutation(jax.random.fold_in(arg_keys[3], 3), NBLK // NB_DEV)
    random_owner = jax.vmap(lambda own, number: assign_block(jax.random.fold_in(arg_keys[3], 2), own, number, NB_DEV, NBLK // NB_DEV, RANDOM, CAP, 2))(random_owner_keys, random_owner_turns).reshape((NBLK, RANDOM))
    random_local = with_ends(jax.random.randint(arg_keys[4], (NBLK, RANDOM), 0, NB_DEV), jax.random.fold_in(arg_keys[4], 1), 0, NB_DEV - 1).astype(jnp.int32)
    output_weight = noise(arg_keys[5], (HEADS * HEAD_DIM, D), (HEADS * HEAD_DIM) ** -0.5, 0.09375, ((0, 4),))
    return dict(queries=queries, key_rows=key_rows, value_rows=value_rows, random_owner=random_owner, random_local=random_local, output_weight=output_weight)


masked_score = -1e30


def sparse_block(block_index, queries, key_padded, value_padded, key_rows, value_rows, random_block):
    score_scale = HEAD_DIM ** -0.5
    first_row = block_index * BLOCK
    query_block = lax.dynamic_slice_in_dim(queries, first_row, BLOCK, 0)
    window_keys = lax.dynamic_slice_in_dim(key_padded, first_row, 3 * BLOCK, 0)
    window_values = lax.dynamic_slice_in_dim(value_padded, first_row, 3 * BLOCK, 0)
    picked = random_block[block_index]
    offsets = (picked[:, None] * BLOCK + jnp.arange(BLOCK, dtype=jnp.int32)[None, :]).reshape(-1).astype(jnp.int32)
    random_keys = jnp.take(key_rows, offsets, axis=0)
    random_values = jnp.take(value_rows, offsets, axis=0)
    listed_keys = jnp.concatenate([window_keys, random_keys, key_rows[:GLOBAL]], axis=0)
    listed_values = jnp.concatenate([window_values, random_values, value_rows[:GLOBAL]], axis=0)
    listed = listed_keys.shape[0]
    slot_number = jnp.arange(listed, dtype=jnp.int32) // BLOCK
    usable = jnp.logical_and(jnp.logical_or(slot_number != 0, block_index > 0), jnp.logical_or(slot_number != 2, block_index < NBLK - 1))
    query_heads = query_block.astype(jnp.float32).reshape(BLOCK, HEADS, HEAD_DIM)
    key_heads = listed_keys.astype(jnp.float32).reshape(listed, HEADS, HEAD_DIM)
    value_heads = listed_values.astype(jnp.float32).reshape(listed, HEADS, HEAD_DIM)
    scores = jnp.einsum("qhd,khd->hqk", query_heads, key_heads) * score_scale
    scores = jnp.where(usable[None, None, :], scores, masked_score)
    row_max = jnp.max(scores, axis=2, keepdims=True)
    weight = jnp.where(usable[None, None, :], jnp.exp(scores - row_max), 0.0)
    row_total = jnp.sum(weight, axis=2)
    rounded = lax.optimization_barrier(weight.astype(jnp.bfloat16)).astype(jnp.float32)
    context = jnp.einsum("hqk,khd->qhd", rounded, value_heads) / jnp.transpose(row_total)[:, :, None]
    return context.reshape(BLOCK, HEADS * HEAD_DIM).astype(jnp.bfloat16)


def segment_part(segment, global_query, key_rows, value_rows):
    segment_rows = NB_DEV * BLOCK
    score_scale = HEAD_DIM ** -0.5
    segment_keys = lax.dynamic_slice_in_dim(key_rows, segment * segment_rows, segment_rows, 0)
    segment_values = lax.dynamic_slice_in_dim(value_rows, segment * segment_rows, segment_rows, 0)
    query_heads = global_query.astype(jnp.float32).reshape(GLOBAL, HEADS, HEAD_DIM)
    key_heads = segment_keys.astype(jnp.float32).reshape(segment_rows, HEADS, HEAD_DIM)
    value_heads = segment_values.astype(jnp.float32).reshape(segment_rows, HEADS, HEAD_DIM)
    scores = jnp.einsum("qhd,khd->hqk", query_heads, key_heads) * score_scale
    row_max = jnp.max(scores, axis=2)
    weight = jnp.exp(scores - row_max[:, :, None])
    row_total = jnp.sum(weight, axis=2)
    rounded = lax.optimization_barrier(weight.astype(jnp.bfloat16)).astype(jnp.float32)
    partial_value = jnp.einsum("hqk,khd->hqd", rounded, value_heads)
    return row_max, row_total, partial_value


def reference(queries, key_rows, value_rows, random_owner, random_local, output_weight):
    random_block = (random_owner * NB_DEV + random_local).astype(jnp.int32)
    total_width = HEADS * HEAD_DIM
    zero_block = jnp.zeros((BLOCK, total_width), key_rows.dtype)
    key_padded = jnp.concatenate([zero_block, key_rows, zero_block], axis=0)
    value_padded = jnp.concatenate([zero_block, value_rows, zero_block], axis=0)

    def one_block(block_index):
        return sparse_block(block_index, queries, key_padded, value_padded, key_rows, value_rows, random_block)

    sparse = lax.map(one_block, jnp.arange(NBLK, dtype=jnp.int32)).reshape(TOKENS, total_width)
    global_query = queries[:GLOBAL]

    def one_segment(segment):
        return segment_part(segment, global_query, key_rows, value_rows)

    segment_max, segment_total, segment_acc = lax.map(one_segment, jnp.arange(N_SEQ, dtype=jnp.int32))
    overall_max = jnp.max(segment_max, axis=0)
    factor = jnp.exp(segment_max - overall_max[None])
    global_out = jnp.sum(factor[..., None] * segment_acc, axis=0) / jnp.sum(factor * segment_total, axis=0)[..., None]
    global_out = jnp.transpose(global_out, (1, 0, 2)).reshape(GLOBAL, total_width)
    attention = jnp.concatenate([global_out.astype(jnp.bfloat16), sparse[GLOBAL:]], axis=0)
    return jnp.dot(attention, output_weight, preferred_element_type=jnp.float32).astype(jnp.bfloat16)
```

```python
import math

import jax
import jax.numpy as jnp
from jax import lax
from jax.experimental import pallas as pl
from jax.experimental.pallas import tpu as pltpu
from jax.sharding import PartitionSpec as P

MESH = pl.DeviceIdType.MESH
HD = 128
BLK = 64
GLOB = 128
ROWS = 1024
WIDTH = 1024
CHUNKS = 4
HPC = 2
CW = HPC * HD
SCALE2 = HD ** (-0.5) * math.log2(math.e)
BF = jnp.bfloat16
F32 = jnp.float32
NT = (((1,), (1,)), ((), ()))
TN = (((0,), (0,)), ((), ()))


def table_kernel(owner, place, reqk, reqv, kidx, vidx, count):
    def clear(i, carry):
        count[i] = 0
        return carry

    lax.fori_loop(0, 32, clear, 0)

    def blank(i, carry):
        reqk[i // 8, 0, i % 8] = 0
        reqv[i // 8, 0, i % 8] = 0
        return carry

    lax.fori_loop(0, 64, blank, 0)

    def fill(i, carry):
        o = owner[i // 3, i % 3]
        p = place[i // 3, i % 3]
        n = count[o]
        count[o] = n + 1
        z, x, c = o // 8, (o // 2) % 4, o % 2
        reqk[x * 2 + c, 0, z * 2 + n] = p
        reqv[z * 2 + c, 0, x * 2 + n] = p
        kidx[i] = (x * 2 + c) * 8 + z * 2 + n
        vidx[i] = (z * 2 + c) * 8 + x * 2 + n
        return carry

    lax.fori_loop(0, 48, fill, 0)


def tables(owner, place):
    smem = pl.BlockSpec(memory_space=pltpu.SMEM)
    i32 = jnp.int32
    return pl.pallas_call(
        table_kernel,
        out_shape=[
            jax.ShapeDtypeStruct((8, 1, 128), i32),
            jax.ShapeDtypeStruct((8, 1, 128), i32),
            jax.ShapeDtypeStruct((48,), i32),
            jax.ShapeDtypeStruct((48,), i32),
        ],
        in_specs=[smem, smem],
        out_specs=[smem] * 4,
        scratch_shapes=[pltpu.SMEM((32,), i32)],
        name="tables",
    )(owner, place)


def main_kernel(
    kidx, vidx, reqk, reqv, q_hbm, k_hbm, v_hbm, w_hbm,
    att_out, wfull,
    kag, vag, kx, vx, qv, stk, stv, rk0, rk1, rk2, rk3, rv0, rv1, rv2, rv3,
    gq, gk, gv, att, part, r1, r2, comb, gout, rqk, rqv, sqk, sqv,
    loc, rq_s, rq_r, ed_s, ed_r, ag_s, ag_r, w_s, w_r, wd_s, wd_r,
    a2_s, a2_r, g_s, g_r, y_s, y_r, r1_s, r1_r, r2_s, r2_r, r3_s, r3_r,
):
    rks, rvs = (rk0, rk1, rk2, rk3), (rv0, rv1, rv2, rv3)
    s = lax.axis_index("seq")
    y = lax.axis_index("head")
    z, x, c = s // 8, (s // 2) % 4, s % 2
    xc, zc = x * 2 + c, z * 2 + c

    def at(dz=0, dx=0, dc=0, dy=0):
        return ((((z + dz) % 4) * 4 + (x + dx) % 4) * 2 + (c + dc) % 2, (y + dy) % 4)

    def remote(src, dst, ss, rs, dev):
        return pltpu.make_async_remote_copy(
            src_ref=src, dst_ref=dst, send_sem=ss, recv_sem=rs, device_id=dev, device_id_type=MESH
        )

    nxt, prv = ((s + 1) % 32, y), ((s + 31) % 32, y)
    row_peers = [(dx, dc) for dx in (1, 3, 2, 0) for dc in (0, 1) if (dx, dc) != (0, 0)]

    own = [
        pltpu.make_async_copy(k_hbm, kag.at[z], loc.at[0]),
        pltpu.make_async_copy(v_hbm, vag.at[x], loc.at[1]),
        pltpu.make_async_copy(k_hbm, kx.at[pl.ds(1, 16)], loc.at[2]),
        pltpu.make_async_copy(v_hbm, vx.at[pl.ds(1, 16)], loc.at[3]),
        pltpu.make_async_copy(q_hbm, qv, loc.at[4]),
    ]
    for cp in own:
        cp.start()

    bar = pltpu.get_barrier_semaphore()
    peers = [at(dx=dx, dc=dc) for dx, dc in row_peers]
    peers += [at(dz=dz, dc=dc) for dz in (1, 2, 3) for dc in (0, 1)]
    peers += [at(dy=dy) for dy in (1, 2, 3)]
    peers += [nxt, prv]
    for dev in peers:
        pl.semaphore_signal(bar, inc=1, device_id=dev, device_id_type=MESH)
    root = jnp.logical_and(s == 0, y == 0)

    @pl.when(z == 0)
    def _():
        @pl.when(jnp.logical_not(root))
        def _():
            pl.semaphore_signal(bar, inc=1, device_id=(0, 0), device_id_type=MESH)

    @pl.when(root)
    def _():
        for ss in range(8):
            for yy in range(4):
                if (ss, yy) != (0, 0):
                    pl.semaphore_signal(bar, inc=1, device_id=(ss, yy), device_id_type=MESH)
        pl.semaphore_wait(bar, len(peers) + 31)

    @pl.when(jnp.logical_not(root))
    def _():
        @pl.when(z == 0)
        def _():
            pl.semaphore_wait(bar, len(peers) + 1)

        @pl.when(z != 0)
        def _():
            pl.semaphore_wait(bar, len(peers))

    late = []

    def go(cp):
        cp.start()
        late.append(cp)
        return cp

    rq = []
    for i, (dx, dc) in enumerate(row_peers):
        tgt = ((x + dx) % 4) * 2 + (c + dc) % 2
        rq.append(go(remote(reqk.at[tgt], rqk.at[xc], rq_s.at[0, i], rq_r.at[0, i], at(dx=dx, dc=dc))))
        tgt = ((z + dx) % 4) * 2 + (c + dc) % 2
        rq.append(go(remote(reqv.at[tgt], rqv.at[zc], rq_s.at[1, i], rq_r.at[1, i], at(dz=dx, dc=dc))))

    is00 = jnp.logical_and(x == 0, c == 0)

    def gcopy(src, dst, n, i, dev):
        return remote(src, dst, g_s.at[n, i], g_r.at[n], dev)

    q_top = q_hbm.at[pl.ds(0, GLOB)]
    q_root = pltpu.make_async_copy(q_top, gq, g_r.at[0])

    @pl.when(s == 0)
    def _():
        q_root.start()
        for dz in (1, 3, 2):
            gcopy(q_top, gq, 0, dz, at(dz=dz)).start()

    edges = []
    for i, (hbm, ext) in enumerate(((k_hbm, kx), (v_hbm, vx))):
        edges.append(go(remote(hbm.at[0], ext.at[17], ed_s.at[i, 0], ed_r.at[i, 0], prv)))
        edges.append(go(remote(hbm.at[15], ext.at[0], ed_s.at[i, 1], ed_r.at[i, 1], nxt)))

    def gather(n, own_view, view, up, down, me, ss, rs):
        a = go(remote(own_view(0), view(me, 0), ss.at[n, 0], rs.at[n, 0], up))
        b = go(remote(own_view(1), view(me, 1), ss.at[n, 1], rs.at[n, 1], down))
        d = go(remote(own_view(1), view(me, 1), ss.at[n, 2], rs.at[n, 2], up))
        e = go(remote(own_view(0), view(me, 0), ss.at[n, 3], rs.at[n, 3], down))
        before, after = (me + 3) % 4, (me + 1) % 4
        f = remote(view(before, 0), view(before, 0), ss.at[n, 4], rs.at[n, 4], up)
        g = remote(view(after, 1), view(after, 1), ss.at[n, 5], rs.at[n, 5], down)
        return a, b, d, e, f, g

    agk = gather(
        0, lambda p: k_hbm.at[pl.ds(p * 8, 8)],
        lambda m, p: kag.at[m, pl.ds(p * 8, 8)], at(dz=1), at(dz=3), z, ag_s, ag_r,
    )
    agv = gather(
        1, lambda p: v_hbm.at[pl.ds(p * 8, 8)],
        lambda m, p: vag.at[m, pl.ds(p * 8, 8)], at(dx=1), at(dx=3), x, ag_s, ag_r,
    )
    half = ROWS // 2
    wq = ROWS // 4

    def wview(m, p):
        return wfull.at[pl.ds(m * ROWS + c * half + p * wq, wq)]

    agw = gather(
        0, lambda p: w_hbm.at[pl.ds(c * half + p * wq, wq)],
        wview, at(dy=1), at(dy=3), y, w_s, w_r,
    )
    mate = at(dc=1)
    wown = go(remote(w_hbm, wfull.at[pl.ds(y * ROWS, ROWS)], wd_s.at[6], wd_r.at[6], mate))

    @pl.when(is00)
    def _():
        @pl.when(s == 0)
        def _():
            q_root.wait()

        @pl.when(s != 0)
        def _():
            gcopy(q_top, gq, 0, 0, at()).wait_recv()

        for dx in (1, 3, 2):
            gcopy(gq, gq, 1, dx, at(dx=dx)).start()

    @pl.when(c == 0)
    def _():
        @pl.when(x != 0)
        def _():
            gcopy(gq, gq, 1, 0, at()).wait_recv()

        gcopy(gq, gq, 2, 0, mate).start()

    @pl.when(c == 1)
    def _():
        gcopy(gq, gq, 2, 0, at()).wait_recv()

    for cp in own:
        cp.wait()

    for cp in rq:
        cp.wait_recv()
    rqk[xc] = reqk[xc]
    rqv[zc] = reqv[zc]
    to_s = [pltpu.make_async_copy(rqk, sqk, loc.at[5]), pltpu.make_async_copy(rqv, sqv, loc.at[6])]

    def glob(h, carry):
        cols = pl.ds(pl.multiple_of(h * HD, HD), HD)
        kk = kx[1:17, :, cols].reshape(ROWS, HD)
        vv = vx[1:17, :, cols].reshape(ROWS, HD)
        st = lax.dot_general(kk, gq[:, cols], NT, preferred_element_type=F32)
        m = jnp.max(st, axis=0, keepdims=True)
        p = jnp.exp2((st - m) * SCALE2)
        l = jnp.sum(p, axis=0, keepdims=True)
        part[h, 0:HD, :] = lax.dot_general(vv, p.astype(BF), TN, preferred_element_type=F32)
        row = lax.broadcasted_iota(jnp.int32, (8, HD), 0)
        part[h, HD:HD + 8, :] = jnp.where(row == 0, m, jnp.where(row == 1, l, 0.0))
        return carry

    lax.fori_loop(0, 8, glob, 0)
    for cp in to_s:
        cp.start()
        cp.wait()

    red1 = []
    for i, (dx, dc) in enumerate(row_peers):
        tgt = ((x + dx) % 4) * 2 + (c + dc) % 2
        red1.append(go(remote(part.at[tgt], r1.at[xc], r1_s.at[i], r1_r.at[i], at(dx=dx, dc=dc))))

    def forward(g):
        a, b, d, e, f, h = g
        a.wait_recv()
        go(f)
        b.wait_recv()
        go(h)

    forward(agk)
    forward(agv)
    for g in (agk, agv):
        a, b, d, e, f, h = g
        for cp in (d, e, f, h):
            cp.wait_recv()

    @pl.when(is00)
    def _():
        for dx in (1, 3, 2):
            gcopy(kag.at[0, pl.ds(0, 2)], gk, 3, dx, at(dx=dx)).start()
        gcopy(kag.at[0, pl.ds(0, 2)], gk, 4, 0, mate).start()
        gk[...] = kag[0, 0:2]

    first = jnp.logical_and(z == 0, c == 0)

    @pl.when(first)
    def _():
        for dz in (1, 3, 2):
            gcopy(vag.at[0, pl.ds(0, 2)], gv, 5, dz, at(dz=dz)).start()
        gcopy(vag.at[0, pl.ds(0, 2)], gv, 6, 0, mate).start()
        gv[...] = vag[0, 0:2]

    def stage(ch, j):
        cols = pl.ds(ch * CW, CW)

        def put(n, carry):
            i, t = n // 8, n % 8
            stk[j, i, t] = kag[t // 2, sqk[i, 0, t], :, cols]
            stv[j, i, t] = vag[t // 2, sqv[i, 0, t], :, cols]
            return carry

        lax.fori_loop(0, 64, put, 0)
        rk, rv = rks[ch], rvs[ch]

        def keep(t, carry):
            rk[xc * 8 + t] = stk[j, xc, t]
            rv[zc * 8 + t] = stv[j, zc, t]
            return carry

        lax.fori_loop(0, 8, keep, 0)

    def exchange(ch, j):
        rk, rv = rks[ch], rvs[ch]
        out = []
        for i, (dx, dc) in enumerate(row_peers):
            tgt = ((x + dx) % 4) * 2 + (c + dc) % 2
            out.append(remote(stk.at[j, tgt], rk.at[pl.ds(xc * 8, 8)], a2_s.at[ch, 0, i], a2_r.at[ch, 0, i], at(dx=dx, dc=dc)))
            tgt = ((z + dx) % 4) * 2 + (c + dc) % 2
            out.append(remote(stv.at[j, tgt], rv.at[pl.ds(zc * 8, 8)], a2_s.at[ch, 1, i], a2_r.at[ch, 1, i], at(dz=dx, dc=dc)))
        for cp in out:
            cp.start()
        return out

    def attend(ch):
        rk, rv = rks[ch], rvs[ch]

        def block(b, carry):
            r0 = pl.multiple_of(b * BLK, BLK)
            lane = lax.broadcasted_iota(jnp.int32, (1, 512), 1)
            no_left = jnp.logical_and(s == 0, b == 0)
            no_right = jnp.logical_and(s == 31, b == 15)
            low = jnp.where(no_left, BLK, 0)
            cut = jnp.where(no_right, 2 * BLK, 3 * BLK)
            gone = jnp.logical_or(lane < low, jnp.logical_and(lane >= cut, lane < 3 * BLK))
            bias = jnp.where(gone, -1e30, 0.0)
            for hh in range(HPC):
                c0 = ch * CW + hh * HD
                q = qv[pl.ds(r0, BLK), c0:c0 + HD]
                ks = [kx[pl.ds(b, 3), :, c0:c0 + HD].reshape(3 * BLK, HD)]
                ks += [rk[kidx[b * 3 + r], :, hh * HD:(hh + 1) * HD] for r in range(3)]
                ks += [gk[:, :, c0:c0 + HD].reshape(GLOB, HD)]
                vs = [vx[pl.ds(b, 3), :, c0:c0 + HD].reshape(3 * BLK, HD)]
                vs += [rv[vidx[b * 3 + r], :, hh * HD:(hh + 1) * HD] for r in range(3)]
                vs += [gv[:, :, c0:c0 + HD].reshape(GLOB, HD)]
                sc = lax.dot_general(q, jnp.concatenate(ks, axis=0), NT, preferred_element_type=F32)
                sc = sc + bias
                m = jnp.max(sc, axis=1, keepdims=True)
                p = jnp.exp2((sc - m) * SCALE2)
                l = jnp.sum(p, axis=1, keepdims=True)
                o = jnp.dot(p.astype(BF), jnp.concatenate(vs, axis=0), preferred_element_type=F32)
                att[pl.ds(r0, BLK), c0:c0 + HD] = (o / l).astype(BF)
            return carry

        lax.fori_loop(0, 16, block, 0)

    ysends = []

    def yparts(ch):
        out = []
        for dy in (1, 3, 2):
            tgt = (y + dy) % 4
            for hf in range(2):
                cp = remote(
                    att.at[pl.ds(tgt * 256 + hf * GLOB, GLOB), pl.ds(ch * CW, CW)],
                    att_out.at[pl.ds(hf * GLOB, GLOB), pl.ds(y * WIDTH + ch * CW, CW)],
                    y_s.at[ch, hf, dy], y_r.at[ch, hf, dy], at(dy=dy),
                )
                skip_send = jnp.logical_and(s == 0, tgt == 0) if hf == 0 else None
                skip_recv = root if hf == 0 else None
                out.append((cp, skip_send, skip_recv))
        for hf in range(2):
            cp = pltpu.make_async_copy(
                att.at[pl.ds(y * 256 + hf * GLOB, GLOB), pl.ds(ch * CW, CW)],
                att_out.at[pl.ds(hf * GLOB, GLOB), pl.ds(y * WIDTH + ch * CW, CW)],
                y_s.at[ch, hf, 0],
            )
            out.append((cp, root if hf == 0 else None, None))
        return out

    def unless(cond, f):
        if cond is None:
            f()
        else:
            pl.when(jnp.logical_not(cond))(f)

    def ysend(ch):
        out = yparts(ch)
        for cp, skip, _ in out:
            unless(skip, cp.start)
        ysends.append(out)

    def weight_forward():
        a, b, d, e, f, g = agw
        a.wait_recv()
        go(f)
        b.wait_recv()
        go(g)

    def wmate(n, m, p):
        return go(remote(wview(m, p), wview(m, p), wd_s.at[n], wd_r.at[n], mate))

    stage(0, 0)
    sent = [exchange(0, 0)]
    stage(1, 1)
    sent.append(exchange(1, 1))
    weight_forward()
    left, right, far = (y + 3) % 4, (y + 1) % 4, (y + 2) % 4
    wm = [wmate(0, left, 0), wmate(1, right, 1)]

    for cp in edges:
        cp.wait_recv()

    @pl.when(jnp.logical_and(c == 0, x != 0))
    def _():
        gcopy(gk, gk, 3, 0, at()).wait_recv()
        gcopy(gk, gk, 4, 0, mate).start()

    @pl.when(jnp.logical_and(c == 0, z != 0))
    def _():
        gcopy(gv, gv, 5, 0, at()).wait_recv()
        gcopy(gv, gv, 6, 0, mate).start()

    @pl.when(c == 1)
    def _():
        gcopy(gk, gk, 4, 0, at()).wait_recv()
        gcopy(gv, gv, 6, 0, at()).wait_recv()

    def arrived(ch):
        for cp in sent[ch]:
            cp.wait_recv()

    def merge(buf, n, dst):
        m = buf[0, HD:HD + 1, :]
        for i in range(1, n):
            m = jnp.maximum(m, buf[i, HD:HD + 1, :])
        l = jnp.zeros((1, HD), F32)
        a = jnp.zeros((HD, HD), F32)
        for i in range(n):
            f = jnp.exp2((buf[i, HD:HD + 1, :] - m) * SCALE2)
            l = l + buf[i, HD + 1:HD + 2, :] * f
            a = a + buf[i, 0:HD, :] * f
        dst(m, l, a)

    arrived(0)
    attend(0)
    for cp in sent[0]:
        cp.wait_send()
    stage(2, 0)
    sent.append(exchange(2, 0))
    ysend(0)

    for cp in red1:
        cp.wait_recv()
    r1[xc] = part[xc]

    def to_comb(m, l, a):
        comb[0:HD, :] = a
        row = lax.broadcasted_iota(jnp.int32, (8, HD), 0)
        comb[HD:HD + 8, :] = jnp.where(row == 0, m, jnp.where(row == 1, l, 0.0))

    merge(r1, 8, to_comb)

    arrived(1)
    attend(1)
    for dz in (1, 2, 3):
        @pl.when(z == dz)
        def _(dz=dz):
            remote(comb, r2.at[dz], r2_s.at[dz], r2_r.at[dz], at(dz=4 - dz)).start()

    for cp in sent[1]:
        cp.wait_send()
    stage(3, 1)
    sent.append(exchange(3, 1))
    ysend(1)
    a, b, d, e, f, g = agw
    d.wait_recv()
    e.wait_recv()
    wm += [wmate(2, left, 1), wmate(3, right, 0)]

    def gplace(yy, hh):
        return att_out.at[pl.ds(0, GLOB), pl.ds(yy * WIDTH + hh * HD, HD)]

    @pl.when(z == 0)
    def _():
        for dz in (1, 2, 3):
            remote(comb, r2.at[dz], r2_s.at[dz], r2_r.at[dz], at()).wait_recv()
        r2[0] = comb[...]

        def finish(m, l, a):
            gout[...] = jnp.transpose(a / l).astype(BF)

        merge(r2, 4, finish)

    arrived(2)
    attend(2)

    @pl.when(z == 0)
    def _():
        @pl.when(root)
        def _():
            pltpu.make_async_copy(gout, gplace(0, 0), r3_r.at[0]).start()

        @pl.when(jnp.logical_not(root))
        def _():
            remote(gout, gplace(y, xc), r3_s, r3_r.at[y * 8 + xc], (0, 0)).start()

    ysend(2)
    f.wait_recv()
    g.wait_recv()
    wm += [wmate(4, far, 0), wmate(5, far, 1)]

    arrived(3)
    attend(3)
    ysend(3)

    for out in ysends:
        for i, (cp, skip_send, skip_recv) in enumerate(out):
            if i < 6:
                unless(skip_send, cp.wait_send)
                unless(skip_recv, cp.wait_recv)
            else:
                unless(skip_send, cp.wait)

    @pl.when(z == 0)
    def _():
        @pl.when(root)
        def _():
            pltpu.make_async_copy(gout, gplace(0, 0), r3_r.at[0]).wait()
            for n in range(1, 32):
                remote(gout, gplace(n // 8, n % 8), r3_s, r3_r.at[n], (0, 0)).wait_recv()

        @pl.when(jnp.logical_not(root))
        def _():
            remote(gout, gplace(y, xc), r3_s, r3_r.at[y * 8 + xc], (0, 0)).wait_send()

    for dz in (1, 2, 3):
        @pl.when(z == dz)
        def _(dz=dz):
            remote(comb, r2.at[dz], r2_s.at[dz], r2_r.at[dz], at(dz=4 - dz)).wait_send()

    wown.wait_recv()
    for cp in wm:
        cp.wait_recv()
    for cp in late:
        cp.wait_send()
    for ch in (2, 3):
        for cp in sent[ch]:
            cp.wait_send()

    @pl.when(s == 0)
    def _():
        for dz in (1, 3, 2):
            gcopy(q_top, gq, 0, dz, at(dz=dz)).wait_send()

    @pl.when(is00)
    def _():
        for dx in (1, 3, 2):
            gcopy(gq, gq, 1, dx, at(dx=dx)).wait_send()
            gcopy(gk, gk, 3, dx, at(dx=dx)).wait_send()

    @pl.when(first)
    def _():
        for dz in (1, 3, 2):
            gcopy(gv, gv, 5, dz, at(dz=dz)).wait_send()

    @pl.when(c == 0)
    def _():
        gcopy(gq, gq, 2, 0, mate).wait_send()
        gcopy(gk, gk, 4, 0, mate).wait_send()
        gcopy(gv, gv, 6, 0, mate).wait_send()


def local(queries, key_rows, value_rows, random_owner, random_local, output_weight):
    reqk, reqv, kidx, vidx = tables(random_owner, random_local)
    smem = pl.BlockSpec(memory_space=pltpu.SMEM)
    vmem = pl.BlockSpec(memory_space=pltpu.VMEM)
    hbm = pl.BlockSpec(memory_space=pl.ANY)
    dma = pltpu.SemaphoreType.DMA
    scratch = [
        pltpu.VMEM((4, 16, BLK, WIDTH), BF),
        pltpu.VMEM((4, 16, BLK, WIDTH), BF),
        pltpu.VMEM((18, BLK, WIDTH), BF),
        pltpu.VMEM((18, BLK, WIDTH), BF),
        pltpu.VMEM((ROWS, WIDTH), BF),
        pltpu.VMEM((2, 8, 8, BLK, CW), BF),
        pltpu.VMEM((2, 8, 8, BLK, CW), BF),
    ]
    scratch += [pltpu.VMEM((64, BLK, CW), BF) for _ in range(8)]
    scratch += [pltpu.VMEM((GLOB, WIDTH), BF)]
    scratch += [pltpu.VMEM((2, BLK, WIDTH), BF) for _ in range(2)]
    scratch += [
        pltpu.VMEM((ROWS, WIDTH), BF),
        pltpu.VMEM((8, HD + 8, HD), F32),
        pltpu.VMEM((8, HD + 8, HD), F32),
        pltpu.VMEM((4, HD + 8, HD), F32),
        pltpu.VMEM((HD + 8, HD), F32),
        pltpu.VMEM((GLOB, HD), BF),
        pltpu.VMEM((8, 1, 128), jnp.int32),
        pltpu.VMEM((8, 1, 128), jnp.int32),
        pltpu.SMEM((8, 1, 128), jnp.int32),
        pltpu.SMEM((8, 1, 128), jnp.int32),
        dma((7,)),
        dma((2, 7)), dma((2, 7)),
        dma((2, 2)), dma((2, 2)),
        dma((2, 6)), dma((2, 6)),
        dma((1, 6)), dma((1, 6)),
        dma((7,)), dma((7,)),
        dma((CHUNKS, 2, 7)), dma((CHUNKS, 2, 7)),
        dma((7, 4)), dma((7,)),
        dma((CHUNKS, 2, 4)), dma((CHUNKS, 2, 4)),
        dma((7,)), dma((7,)),
        dma((4,)), dma((4,)),
        dma, dma((32,)),
    ]
    att, wfull = pl.pallas_call(
        main_kernel,
        out_shape=[
            jax.ShapeDtypeStruct((256, 4096), BF),
            jax.ShapeDtypeStruct((4096, 4096), BF),
        ],
        in_specs=[smem, smem, vmem, vmem, hbm, hbm, hbm, hbm],
        out_specs=[hbm, hbm],
        scratch_shapes=scratch,
        compiler_params=pltpu.CompilerParams(
            collective_id=0, has_side_effects=True, vmem_limit_bytes=63 * 2**20
        ),
        name="exchange_attend",
    )(
        kidx, vidx, reqk, reqv, queries, key_rows.reshape(16, BLK, WIDTH),
        value_rows.reshape(16, BLK, WIDTH), output_weight,
    )
    return jnp.dot(att, wfull, preferred_element_type=F32).astype(BF)


def solution(mesh):
    return jax.shard_map(
        local,
        mesh=mesh,
        in_specs=(
            P("seq", "head"),
            P("seq", "head"),
            P("seq", "head"),
            P("seq", None),
            P("seq", None),
            P("head", None),
        ),
        out_specs=P(("seq", "head"), None),
        check_vma=False,
    )
```

```python
import math

import jax
import jax.numpy as jnp
from jax import lax
from jax.experimental import pallas as pl
from jax.experimental.pallas import tpu as pltpu
from jax.sharding import PartitionSpec as P

MESH = pl.DeviceIdType.MESH
HD = 128
BLK = 64
GLOB = 128
RANDOM = 3
UNITS = 2
ROWS = 1024
WIDTH = 1024
HEADS_OF = ((0, 2), (2, 2), (4, 2), (6, 1), (7, 1))
CHUNKS = len(HEADS_OF)
SCALE2 = HD ** (-0.5) * math.log2(math.e)
BF = jnp.bfloat16
F32 = jnp.float32
NT = (((1,), (1,)), ((), ()))
TN = (((0,), (0,)), ((), ()))


def main_kernel(
    owner, place, q_hbm, k_hbm, v_hbm, w_hbm,
    out_hbm, wfull,
    kag, vag, kx, vx, qv, stk0, stv0, stk1, stv1, stk2, stv2, *rest,
):
    rks, rvs, rest = rest[:CHUNKS], rest[CHUNKS:2 * CHUNKS], rest[2 * CHUNKS:]
    (
        gq, gk, gv, att, atts, acc, outv, part, pml, r1, m1, r2, comb, gout, reqk, reqv, rqk, rqv, sqk, sqv, kidx, vidx,
        loc, rq_s, rq_r, ed_s, ed_r, ag_s, ag_r, w_s, w_r, wd_s, wd_r,
        a2_s, a2_r, g_s, g_r, y_s, y_r, r1_s, r1_r, r2_s, r2_r, r3_s, r3_r, pf, ob,
    ) = rest
    stages = ((stk0, stv0), (stk1, stv1), (stk0, stv0), (stk1, stv1), (stk2, stv2))
    s = lax.axis_index("seq")
    y = lax.axis_index("head")
    z, x, c = s // 8, (s // 2) % 4, s % 2
    xc, zc = x * 2 + c, z * 2 + c

    def at(dz=0, dx=0, dc=0, dy=0):
        return ((((z + dz) % 4) * 4 + (x + dx) % 4) * 2 + (c + dc) % 2, (y + dy) % 4)

    def remote(src, dst, ss, rs, dev):
        return pltpu.make_async_remote_copy(
            src_ref=src, dst_ref=dst, send_sem=ss, recv_sem=rs, device_id=dev, device_id_type=MESH
        )

    def unless(cond, f):
        if cond is None:
            f()
        else:
            pl.when(jnp.logical_not(cond))(f)

    nxt, prv = ((s + 1) % 32, y), ((s + 31) % 32, y)
    row_peers = [(dx, dc) for dx in (1, 3, 2, 0) for dc in (0, 1) if (dx, dc) != (0, 0)]

    own = [
        pltpu.make_async_copy(k_hbm, kag.at[z], loc.at[0]),
        pltpu.make_async_copy(v_hbm, vag.at[x], loc.at[1]),
        pltpu.make_async_copy(k_hbm, kx.at[pl.ds(1, 16)], loc.at[2]),
        pltpu.make_async_copy(v_hbm, vx.at[pl.ds(1, 16)], loc.at[3]),
        pltpu.make_async_copy(q_hbm, qv, loc.at[4]),
    ]
    for cp in own:
        cp.start()

    bar = pltpu.get_barrier_semaphore()
    peers = [at(dx=dx, dc=dc) for dx, dc in row_peers]
    peers += [at(dz=dz, dc=dc) for dz in (1, 2, 3) for dc in (0, 1)]
    peers += [at(dy=dy) for dy in (1, 2, 3)]
    peers += [nxt, prv]
    for dev in peers:
        pl.semaphore_signal(bar, inc=1, device_id=dev, device_id_type=MESH)
    root = jnp.logical_and(s == 0, y == 0)

    @pl.when(z == 0)
    def _():
        @pl.when(jnp.logical_not(root))
        def _():
            pl.semaphore_signal(bar, inc=1, device_id=(0, 0), device_id_type=MESH)

    @pl.when(root)
    def _():
        for ss in range(8):
            for yy in range(4):
                if (ss, yy) != (0, 0):
                    pl.semaphore_signal(bar, inc=1, device_id=(ss, yy), device_id_type=MESH)
        pl.semaphore_wait(bar, len(peers) + 31)

    @pl.when(jnp.logical_not(root))
    def _():
        @pl.when(z == 0)
        def _():
            pl.semaphore_wait(bar, len(peers) + 1)

        @pl.when(z != 0)
        def _():
            pl.semaphore_wait(bar, len(peers))

    late = []

    def go(cp):
        cp.start()
        late.append(cp)
        return cp

    is00 = jnp.logical_and(x == 0, c == 0)
    mate = at(dc=1)

    def gcopy(src, dst, n, i, dev):
        return remote(src, dst, g_s.at[n, i], g_r.at[n], dev)

    q_top = q_hbm.at[pl.ds(0, GLOB)]
    q_root = pltpu.make_async_copy(q_top, gq, g_r.at[0])

    @pl.when(s == 0)
    def _():
        q_root.start()
        for dz in (1, 3, 2):
            gcopy(q_top, gq, 0, dz, at(dz=dz)).start()

    def gather(n, own_view, view, up, down, me, ss, rs):
        a = remote(own_view(0), view(me, 0), ss.at[n, 0], rs.at[n, 0], up)
        b = remote(own_view(1), view(me, 1), ss.at[n, 1], rs.at[n, 1], down)
        d = remote(own_view(1), view(me, 1), ss.at[n, 2], rs.at[n, 2], up)
        e = remote(own_view(0), view(me, 0), ss.at[n, 3], rs.at[n, 3], down)
        before, after = (me + 3) % 4, (me + 1) % 4
        f = remote(view(before, 0), view(before, 0), ss.at[n, 4], rs.at[n, 4], up)
        g = remote(view(after, 1), view(after, 1), ss.at[n, 5], rs.at[n, 5], down)
        return a, b, d, e, f, g

    agk = gather(
        0, lambda p: k_hbm.at[pl.ds(p * 8, 8)],
        lambda m, p: kag.at[m, pl.ds(p * 8, 8)], at(dz=1), at(dz=3), z, ag_s, ag_r,
    )
    agv = gather(
        1, lambda p: v_hbm.at[pl.ds(p * 8, 8)],
        lambda m, p: vag.at[m, pl.ds(p * 8, 8)], at(dx=1), at(dx=3), x, ag_s, ag_r,
    )

    def wview(m, p):
        return wfull.at[pl.ds(m * 16 + c * 8 + p * 4, 4)]

    agw = gather(
        0, lambda p: w_hbm.at[pl.ds(c * 8 + p * 4, 4)],
        wview, at(dy=1), at(dy=3), y, w_s, w_r,
    )
    for n in range(4):
        for g in (agk, agv, agw):
            g[n].start()

    edges = []
    for i, (hbm, ext) in enumerate(((k_hbm, kx), (v_hbm, vx))):
        edges.append(go(remote(hbm.at[0], ext.at[17], ed_s.at[i, 0], ed_r.at[i, 0], prv)))
        edges.append(go(remote(hbm.at[15], ext.at[0], ed_s.at[i, 1], ed_r.at[i, 1], nxt)))

    wown = go(remote(w_hbm, wfull.at[pl.ds(y * 16, 16)], wd_s.at[6], wd_r.at[6], mate))

    @pl.when(is00)
    def _():
        @pl.when(s == 0)
        def _():
            q_root.wait()

        @pl.when(s != 0)
        def _():
            gcopy(q_top, gq, 0, 0, at()).wait_recv()

        for dx in (1, 3, 2):
            gcopy(gq, gq, 1, dx, at(dx=dx)).start()

    reqk[...] = jnp.zeros((8, 1, 128), jnp.int32)
    reqv[...] = jnp.zeros((8, 1, 128), jnp.int32)
    lanes = lax.broadcasted_iota(jnp.int32, (1, 128), 1)

    def serve(o, carry):
        def look(b, st):
            n, p0, p1 = st
            for r in range(RANDOM):
                hit = owner[r, b] == o
                here = place[r, b]
                p0 = jnp.where(jnp.logical_and(hit, n == 0), here, p0)
                p1 = jnp.where(jnp.logical_and(hit, n == 1), here, p1)
                n = n + jnp.where(hit, 1, 0)
            return n, p0, p1

        zero = jnp.int32(0)
        _, p0, p1 = lax.fori_loop(0, 16, look, (zero, zero, zero))
        oz, ox, oc = o // 8, (o // 2) % 4, o % 2

        def row(old, t):
            return jnp.where(lanes == t, p0, jnp.where(lanes == t + 1, p1, old))

        reqk[ox * 2 + oc] = row(reqk[ox * 2 + oc], oz * 2)
        reqv[oz * 2 + oc] = row(reqv[oz * 2 + oc], ox * 2)
        return carry

    lax.fori_loop(0, 32, serve, 0)

    def number(b, carry):
        for r in range(RANDOM):
            o = owner[r, b]

            def before(bb, n):
                for rr in range(RANDOM):
                    n = n + jnp.where(owner[rr, bb] == o, 1, 0)
                return n

            n = lax.fori_loop(0, b, before, jnp.int32(0))
            oz, ox, oc = o // 8, (o // 2) % 4, o % 2
            kidx[b * RANDOM + r] = (ox * 2 + oc) * 8 + oz * 2 + n
            vidx[b * RANDOM + r] = (oz * 2 + oc) * 8 + ox * 2 + n
        return carry

    lax.fori_loop(0, 16, number, 0)

    rq = []
    for i, (dx, dc) in enumerate(row_peers):
        tgt = ((x + dx) % 4) * 2 + (c + dc) % 2
        rq.append(go(remote(reqk.at[tgt], rqk.at[xc], rq_s.at[0, i], rq_r.at[0, i], at(dx=dx, dc=dc))))
        tgt = ((z + dx) % 4) * 2 + (c + dc) % 2
        rq.append(go(remote(reqv.at[tgt], rqv.at[zc], rq_s.at[1, i], rq_r.at[1, i], at(dz=dx, dc=dc))))

    def forward(g):
        g[0].wait_recv()
        g[4].start()
        g[1].wait_recv()
        g[5].start()

    forward(agk)
    forward(agv)
    for cp in own:
        cp.wait()

    @pl.when(c == 0)
    def _():
        @pl.when(x != 0)
        def _():
            gcopy(gq, gq, 1, 0, at()).wait_recv()

        gcopy(gq, gq, 2, 0, mate).start()

    @pl.when(c == 1)
    def _():
        gcopy(gq, gq, 2, 0, at()).wait_recv()

    left, right, far = (y + 3) % 4, (y + 1) % 4, (y + 2) % 4

    def wmate(n, m, p):
        return go(remote(wview(m, p), wview(m, p), wd_s.at[n], wd_r.at[n], mate))

    row8 = lax.broadcasted_iota(jnp.int32, (8, HD), 0)

    def max_total(m, l):
        return jnp.where(row8 == 0, m, jnp.where(row8 == 1, l, 0.0))

    def glob(h, carry):
        cols = pl.ds(pl.multiple_of(h * HD, HD), HD)
        kk = kx[1:17, :, cols].reshape(ROWS, HD)
        vv = vx[1:17, :, cols].reshape(ROWS, HD)
        st = lax.dot_general(kk, gq[:, cols], NT, preferred_element_type=F32)
        m = jnp.max(st, axis=0, keepdims=True)
        p = jnp.exp2((st - m) * SCALE2)
        l = jnp.sum(p, axis=0, keepdims=True)
        part[h] = lax.dot_general(vv, p.astype(BF), TN, preferred_element_type=F32).astype(BF)
        pml[h] = max_total(m, l)
        return carry

    lax.fori_loop(0, 8, glob, 0)

    forward(agw)
    wm = [wmate(0, left, 0), wmate(1, right, 1)]

    red1 = []
    for i, (dx, dc) in enumerate(row_peers):
        tgt = ((x + dx) % 4) * 2 + (c + dc) % 2
        red1.append(go(remote(part.at[tgt], r1.at[xc], r1_s.at[0, i], r1_r.at[0, i], at(dx=dx, dc=dc))))
        red1.append(go(remote(pml.at[tgt], m1.at[xc], r1_s.at[1, i], r1_r.at[1, i], at(dx=dx, dc=dc))))

    for cp in rq:
        cp.wait_recv()
    rqk[xc] = reqk[xc]
    rqv[zc] = reqv[zc]
    to_s = [pltpu.make_async_copy(rqk, sqk, loc.at[5]), pltpu.make_async_copy(rqv, sqv, loc.at[6])]
    for cp in to_s:
        cp.start()
    for cp in to_s:
        cp.wait()

    for g in (agk, agv):
        for cp in g[2:]:
            cp.wait_recv()

    @pl.when(is00)
    def _():
        for dx in (1, 3, 2):
            gcopy(kag.at[0, pl.ds(0, 2)], gk, 3, dx, at(dx=dx)).start()
        gcopy(kag.at[0, pl.ds(0, 2)], gk, 4, 0, mate).start()
        gk[...] = kag[0, 0:2]

    first = jnp.logical_and(z == 0, c == 0)

    @pl.when(first)
    def _():
        for dz in (1, 3, 2):
            gcopy(vag.at[0, pl.ds(0, 2)], gv, 5, dz, at(dz=dz)).start()
        gcopy(vag.at[0, pl.ds(0, 2)], gv, 6, 0, mate).start()
        gv[...] = vag[0, 0:2]

    def stage(ch):
        h0, nh = HEADS_OF[ch]
        cols, wide = pl.ds(h0 * HD, nh * HD), pl.ds(0, nh * HD)
        stk, stv = stages[ch]
        rk, rv = rks[ch], rvs[ch]

        def put(i, carry):
            for t in range(8):
                stk[i, t, :, wide] = kag[t // 2, sqk[i, 0, t], :, cols]
                stv[i, t, :, wide] = vag[t // 2, sqv[i, 0, t], :, cols]
            return carry

        lax.fori_loop(0, 8, put, 0)

        def keep(t, carry):
            rk[xc * 8 + t] = stk[xc, t, :, wide]
            rv[zc * 8 + t] = stv[zc, t, :, wide]
            return carry

        lax.fori_loop(0, 8, keep, 0)

    def exchange(ch):
        nh = HEADS_OF[ch][1]
        wide = pl.ds(0, nh * HD)
        stk, stv = stages[ch]
        rk, rv = rks[ch], rvs[ch]
        out = []
        for i, (dx, dc) in enumerate(row_peers):
            tgt = ((x + dx) % 4) * 2 + (c + dc) % 2
            out.append(remote(stk.at[tgt, :, :, wide], rk.at[pl.ds(xc * 8, 8)], a2_s.at[ch, 0, i], a2_r.at[ch, 0, i], at(dx=dx, dc=dc)))
            tgt = ((z + dx) % 4) * 2 + (c + dc) % 2
            out.append(remote(stv.at[tgt, :, :, wide], rv.at[pl.ds(zc * 8, 8)], a2_s.at[ch, 1, i], a2_r.at[ch, 1, i], at(dz=dx, dc=dc)))
        for cp in out:
            cp.start()
        return out

    def attend(ch, lo=0, hi=16):
        h0, nh = HEADS_OF[ch]
        rk, rv = rks[ch], rvs[ch]
        lane = lax.broadcasted_iota(jnp.int32, (1, 512), 1)

        def unit(b, bias, hh):
            c0 = (h0 + hh) * HD
            cc = slice(hh * HD, (hh + 1) * HD)
            q = qv[pl.ds(pl.multiple_of(b * BLK, BLK), BLK), c0:c0 + HD]
            ks = [kx[pl.ds(b, 3), :, c0:c0 + HD].reshape(3 * BLK, HD)]
            ks += [rk[kidx[b * RANDOM + r], :, cc] for r in range(RANDOM)]
            ks += [gk[:, :, c0:c0 + HD].reshape(GLOB, HD)]
            vs = [vx[pl.ds(b, 3), :, c0:c0 + HD].reshape(3 * BLK, HD)]
            vs += [rv[vidx[b * RANDOM + r], :, cc] for r in range(RANDOM)]
            vs += [gv[:, :, c0:c0 + HD].reshape(GLOB, HD)]
            sc = lax.dot_general(q, jnp.concatenate(ks, axis=0), NT, preferred_element_type=F32)
            sc = sc + bias
            m = jnp.max(sc, axis=1, keepdims=True)
            p = jnp.exp2((sc - m) * SCALE2)
            l = jnp.sum(p, axis=1, keepdims=True)
            o = jnp.dot(p.astype(BF), jnp.concatenate(vs, axis=0), preferred_element_type=F32)
            att[pl.ds(pl.multiple_of(b * BLK, BLK), BLK), c0:c0 + HD] = (o / l).astype(BF)

        per = UNITS // nh

        def block(bb, carry):
            for k in range(per):
                b = bb * per + k
                no_left = jnp.logical_and(s == 0, b == 0)
                no_right = jnp.logical_and(s == 31, b == 15)
                low = jnp.where(no_left, BLK, 0)
                cut = jnp.where(no_right, 2 * BLK, 3 * BLK)
                gone = jnp.logical_or(lane < low, jnp.logical_and(lane >= cut, lane < 3 * BLK))
                bias = jnp.where(gone, -1e30, 0.0)
                for hh in range(nh):
                    unit(b, bias, hh)
            return carry

        lax.fori_loop(lo // per, hi // per, block, 0)

    ysends = []

    def ysend(ch):
        h0, nh = HEADS_OF[ch]
        out = []
        for h in range(h0, h0 + nh):
            for dy in (1, 3, 2):
                tgt = (y + dy) % 4
                for hf in range(2):
                    cp = remote(
                        att.at[pl.ds(tgt * 256 + hf * GLOB, GLOB), pl.ds(h * HD, HD)],
                        atts.at[h, pl.ds(hf * GLOB, GLOB), pl.ds(y * HD, HD)],
                        y_s.at[h, hf, dy], y_r.at[h, hf, dy], at(dy=dy),
                    )
                    skip = jnp.logical_and(s == 0, tgt == 0) if hf == 0 else None
                    out.append((cp, skip, root if hf == 0 else None))
        for cp, skip, _ in out:
            unless(skip, cp.start)

        def keep(hf):
            rows = pl.ds(pl.multiple_of(y * 256 + hf * GLOB, GLOB), GLOB)
            for h in range(h0, h0 + nh):
                atts[h, hf * GLOB:(hf + 1) * GLOB, pl.ds(pl.multiple_of(y * HD, HD), HD)] = att[rows, h * HD:(h + 1) * HD]

        keep(1)
        unless(root, lambda: keep(0))
        ysends.append(out)

    def yrecv(ch):
        for cp, _, skip in ysends[ch]:
            unless(skip, cp.wait_recv)

    wbufs = ((kag, 0), (vag, 0), (kag, 0), (vag, 0), (vag, 8))

    def prefetch(ch):
        h0, nh = HEADS_OF[ch]
        buf, base = wbufs[ch]
        out = []
        for h in range(nh):
            for yy in range(4):
                for n in range(4):
                    out.append(pltpu.make_async_copy(
                        wfull.at[pl.ds(yy * 16 + (h0 + h) * 2, 2), :, pl.ds(n * WIDTH, WIDTH)],
                        buf.at[n, pl.ds(base + h * 8 + yy * 2, 2)], pf.at[h0 + h, yy * 4 + n],
                    ))
        for cp in out:
            cp.start(priority=1)
        return out

    def project(ch, copies):
        h0, nh = HEADS_OF[ch]
        buf, base = wbufs[ch]
        for cp in copies:
            cp.wait()

        def tile(j, carry):
            n, sub = j // 4, j % 4
            cols = pl.ds(pl.multiple_of(j * 256, 256), 256)
            w = buf[n, base:base + nh * 8, :, pl.ds(pl.multiple_of(sub * 256, 256), 256)].reshape(nh * 512, 256)
            rows = jnp.concatenate([atts[h] for h in range(h0, h0 + nh)], axis=1)
            t = jnp.dot(rows, w, preferred_element_type=F32)
            if ch == 0:
                acc[:, cols] = t
            elif ch < CHUNKS - 1:
                acc[:, cols] += t
            else:
                outv[:, cols] = (acc[:, cols] + t).astype(BF)
            return carry

        lax.fori_loop(0, 16, tile, 0)

    def merge(ml, part_of, n):
        m = ml(0)[0:1, :]
        for i in range(1, n):
            m = jnp.maximum(m, ml(i)[0:1, :])
        l = jnp.zeros((1, HD), F32)
        a = jnp.zeros((HD, HD), F32)
        for i in range(n):
            f = jnp.exp2((ml(i)[0:1, :] - m) * SCALE2)
            l = l + ml(i)[1:2, :] * f
            a = a + part_of(i) * f
        return m, l, a

    stage(0)
    sent = [exchange(0)]
    for cp in red1:
        cp.wait_recv()
    r1[xc] = part[xc]
    m1[xc] = pml[xc]
    m, l, a = merge(lambda i: m1[i], lambda i: r1[i].astype(F32), 8)
    comb[0:HD, :] = a
    comb[HD:HD + 8, :] = max_total(m, l)

    stage(1)
    for dz in (1, 2, 3):
        @pl.when(z == dz)
        def _(dz=dz):
            remote(comb, r2.at[dz], r2_s.at[dz], r2_r.at[dz], at(dz=4 - dz)).start()

    sent.append(exchange(1))
    stage(4)

    for cp in edges:
        cp.wait_recv()

    @pl.when(jnp.logical_and(c == 0, x != 0))
    def _():
        gcopy(gk, gk, 3, 0, at()).wait_recv()
        gcopy(gk, gk, 4, 0, mate).start()

    @pl.when(jnp.logical_and(c == 0, z != 0))
    def _():
        gcopy(gv, gv, 5, 0, at()).wait_recv()
        gcopy(gv, gv, 6, 0, mate).start()

    @pl.when(c == 1)
    def _():
        gcopy(gk, gk, 4, 0, at()).wait_recv()
        gcopy(gv, gv, 6, 0, at()).wait_recv()

    def arrived(ch):
        for cp in sent[ch]:
            cp.wait_recv()

    def refill(ch):
        for cp in sent[ch - 2]:
            cp.wait_send()
        stage(ch)
        sent.append(exchange(ch))

    agw[2].wait_recv()
    agw[3].wait_recv()
    wm += [wmate(2, left, 1), wmate(3, right, 0)]
    arrived(0)
    @pl.when(z == 0)
    def _():
        for dz in (1, 2, 3):
            remote(comb, r2.at[dz], r2_s.at[dz], r2_r.at[dz], at()).wait_recv()
        r2[0] = comb[...]
        _, l, a = merge(lambda i: r2[i, HD:HD + 8, :], lambda i: r2[i, 0:HD, :], 4)
        gout[...] = jnp.transpose(a / l).astype(BF)

    for cp in sent[0]:
        cp.wait_send()
    stage(2)
    def gfinal(yy, hh):
        return remote(gout, atts.at[hh, pl.ds(0, GLOB), pl.ds(yy * HD, HD)], r3_s, r3_r.at[yy * 8 + hh], (0, 0))

    @pl.when(z == 0)
    def _():
        @pl.when(root)
        def _():
            atts[0, 0:GLOB, 0:HD] = gout[...]

        unless(root, lambda: gfinal(y, xc).start())

    sent.append(exchange(2))
    attend(0)
    ysend(0)

    arrived(1)
    refill(3)
    sent.append(exchange(4))
    agw[4].wait_recv()
    agw[5].wait_recv()
    wm += [wmate(4, far, 0), wmate(5, far, 1)]
    attend(1)
    ysend(1)

    for g in (agk, agv):
        for cp in g:
            cp.wait_send()

    @pl.when(is00)
    def _():
        for dx in (1, 3, 2):
            gcopy(gk, gk, 3, dx, at(dx=dx)).wait_send()

    @pl.when(first)
    def _():
        for dz in (1, 3, 2):
            gcopy(gv, gv, 5, dz, at(dz=dz)).wait_send()

    @pl.when(c == 0)
    def _():
        gcopy(gk, gk, 4, 0, mate).wait_send()
        gcopy(gv, gv, 6, 0, mate).wait_send()

    wown.wait_recv()
    for cp in wm:
        cp.wait_recv()
    p0 = prefetch(0)
    p1 = prefetch(1)

    @pl.when(root)
    def _():
        for n in range(1, 32):
            gfinal(n // 8, n % 8).wait_recv()

    yrecv(0)
    project(0, p0)
    p2 = prefetch(2)
    yrecv(1)
    project(1, p1)
    p3 = prefetch(3)
    p4 = prefetch(4)
    arrived(2)
    attend(2)
    ysend(2)
    arrived(3)
    attend(3)
    ysend(3)
    yrecv(2)
    project(2, p2)
    arrived(4)
    attend(4)
    ysend(4)
    yrecv(3)
    project(3, p3 + p4)
    yrecv(4)
    project(4, [])
    done = pltpu.make_async_copy(outv, out_hbm, ob)
    done.start()

    for out in ysends:
        for cp, skip, _ in out:
            unless(skip, cp.wait_send)

    @pl.when(z == 0)
    def _():
        unless(root, lambda: gfinal(y, xc).wait_send())

    for dz in (1, 2, 3):
        @pl.when(z == dz)
        def _(dz=dz):
            remote(comb, r2.at[dz], r2_s.at[dz], r2_r.at[dz], at(dz=4 - dz)).wait_send()

    for cp in late:
        cp.wait_send()
    for cp in agw:
        cp.wait_send()
    for ch in (2, 3, 4):
        for cp in sent[ch]:
            cp.wait_send()

    @pl.when(s == 0)
    def _():
        for dz in (1, 3, 2):
            gcopy(q_top, gq, 0, dz, at(dz=dz)).wait_send()

    @pl.when(is00)
    def _():
        for dx in (1, 3, 2):
            gcopy(gq, gq, 1, dx, at(dx=dx)).wait_send()

    @pl.when(c == 0)
    def _():
        gcopy(gq, gq, 2, 0, mate).wait_send()

    done.wait()


def local(queries, key_rows, value_rows, random_owner, random_local, output_weight):
    smem = pl.BlockSpec(memory_space=pltpu.SMEM)
    hbm = pl.BlockSpec(memory_space=pl.ANY)
    dma = pltpu.SemaphoreType.DMA
    widest = max(nh for _, nh in HEADS_OF) * HD
    scratch = [
        pltpu.VMEM((4, 16, BLK, WIDTH), BF),
        pltpu.VMEM((4, 16, BLK, WIDTH), BF),
        pltpu.VMEM((18, BLK, WIDTH), BF),
        pltpu.VMEM((18, BLK, WIDTH), BF),
        pltpu.VMEM((ROWS, WIDTH), BF),
    ]
    scratch += [pltpu.VMEM((8, 8, BLK, widest), BF) for _ in range(4)]
    scratch += [pltpu.VMEM((8, 8, BLK, HEADS_OF[-1][1] * HD), BF) for _ in range(2)]
    scratch += [pltpu.VMEM((64, BLK, nh * HD), BF) for _ in range(2) for _, nh in HEADS_OF]
    scratch += [pltpu.VMEM((GLOB, WIDTH), BF)]
    scratch += [pltpu.VMEM((2, BLK, WIDTH), BF) for _ in range(2)]
    scratch += [
        pltpu.VMEM((ROWS, WIDTH), BF),
        pltpu.VMEM((8, 256, 512), BF),
        pltpu.VMEM((256, 4096), F32),
        pltpu.VMEM((256, 4096), BF),
        pltpu.VMEM((8, HD, HD), BF),
        pltpu.VMEM((8, 8, HD), F32),
        pltpu.VMEM((8, HD, HD), BF),
        pltpu.VMEM((8, 8, HD), F32),
        pltpu.VMEM((4, HD + 8, HD), F32),
        pltpu.VMEM((HD + 8, HD), F32),
        pltpu.VMEM((GLOB, HD), BF),
        pltpu.VMEM((8, 1, 128), jnp.int32),
        pltpu.VMEM((8, 1, 128), jnp.int32),
        pltpu.VMEM((8, 1, 128), jnp.int32),
        pltpu.VMEM((8, 1, 128), jnp.int32),
        pltpu.SMEM((8, 1, 128), jnp.int32),
        pltpu.SMEM((8, 1, 128), jnp.int32),
        pltpu.SMEM((16 * RANDOM,), jnp.int32),
        pltpu.SMEM((16 * RANDOM,), jnp.int32),
        dma((7,)),
        dma((2, 7)), dma((2, 7)),
        dma((2, 2)), dma((2, 2)),
        dma((2, 6)), dma((2, 6)),
        dma((1, 6)), dma((1, 6)),
        dma((7,)), dma((7,)),
        dma((CHUNKS, 2, 7)), dma((CHUNKS, 2, 7)),
        dma((7, 4)), dma((7,)),
        dma((8, 2, 4)), dma((8, 2, 4)),
        dma((2, 7)), dma((2, 7)),
        dma((4,)), dma((4,)),
        dma, dma((32,)),
        dma((8, 16)), dma,
    ]
    out, _ = pl.pallas_call(
        main_kernel,
        out_shape=[
            jax.ShapeDtypeStruct((256, 4096), BF),
            jax.ShapeDtypeStruct((64, BLK, 4096), BF),
        ],
        in_specs=[smem, smem, hbm, hbm, hbm, hbm],
        out_specs=[hbm, hbm],
        scratch_shapes=scratch,
        compiler_params=pltpu.CompilerParams(
            collective_id=0, has_side_effects=True, vmem_limit_bytes=67043328
        ),
        name="bigbird_layer",
    )(
        random_owner.T, random_local.T, queries, key_rows.reshape(16, BLK, WIDTH),
        value_rows.reshape(16, BLK, WIDTH), output_weight.reshape(16, BLK, 4096),
    )
    return out


def solution(mesh):
    return jax.shard_map(
        local,
        mesh=mesh,
        in_specs=(
            P("seq", "head"),
            P("seq", "head"),
            P("seq", "head"),
            P("seq", None),
            P("seq", None),
            P("head", None),
        ),
        out_specs=P(("seq", "head"), None),
        check_vma=False,
    )
```

```python
import math

import jax
import jax.numpy as jnp
from jax import lax
from jax.experimental import pallas as pl
from jax.experimental.pallas import tpu as pltpu
from jax.sharding import PartitionSpec as P

MESH = pl.DeviceIdType.MESH
HD = 128
BLK = 64
GLOB = 128
RANDOM = 3
UNITS = 8
ROWS = 1024
WIDTH = 1024
HEADS_OF = ((0, 2), (2, 2), (4, 2), (6, 1), (7, 1))
CHUNKS = len(HEADS_OF)
SCALE2 = HD ** (-0.5) * math.log2(math.e)
BF = jnp.bfloat16
F32 = jnp.float32
NT = (((1,), (1,)), ((), ()))
TN = (((0,), (0,)), ((), ()))


def main_kernel(
    owner, place, q_hbm, k_hbm, v_hbm, w_hbm,
    out_hbm, wfull,
    kag, vag, kx, vx, qv, stk0, stv0, stk1, stv1, stk2, stv2, *rest,
):
    rks, rvs, rest = rest[:CHUNKS], rest[CHUNKS:2 * CHUNKS], rest[2 * CHUNKS:]
    (
        gq, gk, gv, att, atts, acc, outv, part, pml, r1, m1, r2, comb, gout, reqk, reqv, rqk, rqv, sqk, sqv, kidx, vidx,
        loc, rq_s, rq_r, ed_s, ed_r, ag_s, ag_r, w_s, w_r, wd_s, wd_r,
        a2_s, a2_r, g_s, g_r, y_s, y_r, r1_s, r1_r, r2_s, r2_r, r3_s, r3_r, pf, ob,
    ) = rest
    stages = ((stk0, stv0), (stk1, stv1), (stk0, stv0), (stk1, stv1), (stk2, stv2))
    s = lax.axis_index("seq")
    y = lax.axis_index("head")
    z, x, c = s // 8, (s // 2) % 4, s % 2
    xc, zc = x * 2 + c, z * 2 + c

    def at(dz=0, dx=0, dc=0, dy=0):
        return ((((z + dz) % 4) * 4 + (x + dx) % 4) * 2 + (c + dc) % 2, (y + dy) % 4)

    def remote(src, dst, ss, rs, dev):
        return pltpu.make_async_remote_copy(
            src_ref=src, dst_ref=dst, send_sem=ss, recv_sem=rs, device_id=dev, device_id_type=MESH
        )

    def unless(cond, f):
        if cond is None:
            f()
        else:
            pl.when(jnp.logical_not(cond))(f)

    nxt, prv = ((s + 1) % 32, y), ((s + 31) % 32, y)
    row_peers = [(dx, dc) for dx in (1, 3, 2, 0) for dc in (0, 1) if (dx, dc) != (0, 0)]

    own = [
        pltpu.make_async_copy(k_hbm, kag.at[z], loc.at[0]),
        pltpu.make_async_copy(v_hbm, vag.at[x], loc.at[1]),
        pltpu.make_async_copy(k_hbm, kx.at[pl.ds(1, 16)], loc.at[2]),
        pltpu.make_async_copy(v_hbm, vx.at[pl.ds(1, 16)], loc.at[3]),
        pltpu.make_async_copy(q_hbm, qv, loc.at[4]),
    ]
    for cp in own:
        cp.start()

    bar = pltpu.get_barrier_semaphore()
    peers = [at(dx=dx, dc=dc) for dx, dc in row_peers]
    peers += [at(dz=dz, dc=dc) for dz in (1, 2, 3) for dc in (0, 1)]
    peers += [at(dy=dy) for dy in (1, 2, 3)]
    peers += [nxt, prv]
    for dev in peers:
        pl.semaphore_signal(bar, inc=1, device_id=dev, device_id_type=MESH)
    root = jnp.logical_and(s == 0, y == 0)

    @pl.when(z == 0)
    def _():
        @pl.when(jnp.logical_not(root))
        def _():
            pl.semaphore_signal(bar, inc=1, device_id=(0, 0), device_id_type=MESH)

    @pl.when(root)
    def _():
        for ss in range(8):
            for yy in range(4):
                if (ss, yy) != (0, 0):
                    pl.semaphore_signal(bar, inc=1, device_id=(ss, yy), device_id_type=MESH)
        pl.semaphore_wait(bar, len(peers) + 31)

    @pl.when(jnp.logical_not(root))
    def _():
        @pl.when(z == 0)
        def _():
            pl.semaphore_wait(bar, len(peers) + 1)

        @pl.when(z != 0)
        def _():
            pl.semaphore_wait(bar, len(peers))

    late = []

    def go(cp):
        cp.start()
        late.append(cp)
        return cp

    is00 = jnp.logical_and(x == 0, c == 0)
    mate = at(dc=1)

    def gcopy(src, dst, n, i, dev):
        return remote(src, dst, g_s.at[n, i], g_r.at[n], dev)

    q_top = q_hbm.at[pl.ds(0, GLOB)]
    q_root = pltpu.make_async_copy(q_top, gq, g_r.at[0])

    @pl.when(s == 0)
    def _():
        q_root.start()
        for dz in (1, 3, 2):
            gcopy(q_top, gq, 0, dz, at(dz=dz)).start()

    def gather(n, own_view, view, up, down, me, ss, rs):
        a = remote(own_view(0), view(me, 0), ss.at[n, 0], rs.at[n, 0], up)
        b = remote(own_view(1), view(me, 1), ss.at[n, 1], rs.at[n, 1], down)
        d = remote(own_view(1), view(me, 1), ss.at[n, 2], rs.at[n, 2], up)
        e = remote(own_view(0), view(me, 0), ss.at[n, 3], rs.at[n, 3], down)
        before, after = (me + 3) % 4, (me + 1) % 4
        f = remote(view(before, 0), view(before, 0), ss.at[n, 4], rs.at[n, 4], up)
        g = remote(view(after, 1), view(after, 1), ss.at[n, 5], rs.at[n, 5], down)
        return a, b, d, e, f, g

    agk = gather(
        0, lambda p: k_hbm.at[pl.ds(p * 8, 8)],
        lambda m, p: kag.at[m, pl.ds(p * 8, 8)], at(dz=1), at(dz=3), z, ag_s, ag_r,
    )
    agv = gather(
        1, lambda p: v_hbm.at[pl.ds(p * 8, 8)],
        lambda m, p: vag.at[m, pl.ds(p * 8, 8)], at(dx=1), at(dx=3), x, ag_s, ag_r,
    )

    def wview(m, p):
        return wfull.at[pl.ds(m * 16 + c * 8 + p * 4, 4)]

    agw = gather(
        0, lambda p: w_hbm.at[pl.ds(c * 8 + p * 4, 4)],
        wview, at(dy=1), at(dy=3), y, w_s, w_r,
    )
    for n in range(4):
        for g in (agk, agv, agw):
            g[n].start()

    edges = []
    for i, (hbm, ext) in enumerate(((k_hbm, kx), (v_hbm, vx))):
        edges.append(go(remote(hbm.at[0], ext.at[17], ed_s.at[i, 0], ed_r.at[i, 0], prv)))
        edges.append(go(remote(hbm.at[15], ext.at[0], ed_s.at[i, 1], ed_r.at[i, 1], nxt)))

    wown = go(remote(w_hbm, wfull.at[pl.ds(y * 16, 16)], wd_s.at[6], wd_r.at[6], mate))

    @pl.when(is00)
    def _():
        @pl.when(s == 0)
        def _():
            q_root.wait()

        @pl.when(s != 0)
        def _():
            gcopy(q_top, gq, 0, 0, at()).wait_recv()

        for dx in (1, 3, 2):
            gcopy(gq, gq, 1, dx, at(dx=dx)).start()

    reqk[...] = jnp.zeros((8, 1, 128), jnp.int32)
    reqv[...] = jnp.zeros((8, 1, 128), jnp.int32)
    lanes = lax.broadcasted_iota(jnp.int32, (1, 128), 1)

    def serve(o, carry):
        def look(b, st):
            n, p0, p1 = st
            for r in range(RANDOM):
                hit = owner[r, b] == o
                here = place[r, b]
                p0 = jnp.where(jnp.logical_and(hit, n == 0), here, p0)
                p1 = jnp.where(jnp.logical_and(hit, n == 1), here, p1)
                n = n + jnp.where(hit, 1, 0)
            return n, p0, p1

        zero = jnp.int32(0)
        _, p0, p1 = lax.fori_loop(0, 16, look, (zero, zero, zero))
        oz, ox, oc = o // 8, (o // 2) % 4, o % 2

        def row(old, t):
            return jnp.where(lanes == t, p0, jnp.where(lanes == t + 1, p1, old))

        reqk[ox * 2 + oc] = row(reqk[ox * 2 + oc], oz * 2)
        reqv[oz * 2 + oc] = row(reqv[oz * 2 + oc], ox * 2)
        return carry

    lax.fori_loop(0, 32, serve, 0)

    def number(b, carry):
        for r in range(RANDOM):
            o = owner[r, b]

            def before(bb, n):
                for rr in range(RANDOM):
                    n = n + jnp.where(owner[rr, bb] == o, 1, 0)
                return n

            n = lax.fori_loop(0, b, before, jnp.int32(0))
            oz, ox, oc = o // 8, (o // 2) % 4, o % 2
            kidx[b * RANDOM + r] = (ox * 2 + oc) * 8 + oz * 2 + n
            vidx[b * RANDOM + r] = (oz * 2 + oc) * 8 + ox * 2 + n
        return carry

    lax.fori_loop(0, 16, number, 0)

    rq = []
    for i, (dx, dc) in enumerate(row_peers):
        tgt = ((x + dx) % 4) * 2 + (c + dc) % 2
        rq.append(go(remote(reqk.at[tgt], rqk.at[xc], rq_s.at[0, i], rq_r.at[0, i], at(dx=dx, dc=dc))))
        tgt = ((z + dx) % 4) * 2 + (c + dc) % 2
        rq.append(go(remote(reqv.at[tgt], rqv.at[zc], rq_s.at[1, i], rq_r.at[1, i], at(dz=dx, dc=dc))))

    def forward(g):
        g[0].wait_recv()
        g[4].start()
        g[1].wait_recv()
        g[5].start()

    forward(agk)
    forward(agv)
    for cp in own:
        cp.wait()

    @pl.when(c == 0)
    def _():
        @pl.when(x != 0)
        def _():
            gcopy(gq, gq, 1, 0, at()).wait_recv()

        gcopy(gq, gq, 2, 0, mate).start()

    @pl.when(c == 1)
    def _():
        gcopy(gq, gq, 2, 0, at()).wait_recv()

    left, right, far = (y + 3) % 4, (y + 1) % 4, (y + 2) % 4

    def wmate(n, m, p):
        return go(remote(wview(m, p), wview(m, p), wd_s.at[n], wd_r.at[n], mate))

    row8 = lax.broadcasted_iota(jnp.int32, (8, HD), 0)

    def max_total(m, l):
        return jnp.where(row8 == 0, m, jnp.where(row8 == 1, l, 0.0))

    def glob(h, carry):
        cols = pl.ds(pl.multiple_of(h * HD, HD), HD)
        kk = kx[1:17, :, cols].reshape(ROWS, HD)
        vv = vx[1:17, :, cols].reshape(ROWS, HD)
        st = lax.dot_general(kk, gq[:, cols], NT, preferred_element_type=F32)
        m = jnp.max(st, axis=0, keepdims=True)
        p = jnp.exp2((st - m) * SCALE2)
        l = jnp.sum(p, axis=0, keepdims=True)
        part[h] = lax.dot_general(vv, p.astype(BF), TN, preferred_element_type=F32).astype(BF)
        pml[h] = max_total(m, l)
        return carry

    lax.fori_loop(0, 8, glob, 0)

    forward(agw)
    wm = [wmate(0, left, 0), wmate(1, right, 1)]

    red1 = []
    for i, (dx, dc) in enumerate(row_peers):
        tgt = ((x + dx) % 4) * 2 + (c + dc) % 2
        red1.append(go(remote(part.at[tgt], r1.at[xc], r1_s.at[0, i], r1_r.at[0, i], at(dx=dx, dc=dc))))
        red1.append(go(remote(pml.at[tgt], m1.at[xc], r1_s.at[1, i], r1_r.at[1, i], at(dx=dx, dc=dc))))

    for cp in rq:
        cp.wait_recv()
    rqk[xc] = reqk[xc]
    rqv[zc] = reqv[zc]
    to_s = [pltpu.make_async_copy(rqk, sqk, loc.at[5]), pltpu.make_async_copy(rqv, sqv, loc.at[6])]
    for cp in to_s:
        cp.start()
    for cp in to_s:
        cp.wait()

    for g in (agk, agv):
        for cp in g[2:]:
            cp.wait_recv()

    @pl.when(is00)
    def _():
        for dx in (1, 3, 2):
            gcopy(kag.at[0, pl.ds(0, 2)], gk, 3, dx, at(dx=dx)).start()
        gcopy(kag.at[0, pl.ds(0, 2)], gk, 4, 0, mate).start()
        gk[...] = kag[0, 0:2]

    first = jnp.logical_and(z == 0, c == 0)

    @pl.when(first)
    def _():
        for dz in (1, 3, 2):
            gcopy(vag.at[0, pl.ds(0, 2)], gv, 5, dz, at(dz=dz)).start()
        gcopy(vag.at[0, pl.ds(0, 2)], gv, 6, 0, mate).start()
        gv[...] = vag[0, 0:2]

    def stage(ch):
        h0, nh = HEADS_OF[ch]
        cols, wide = pl.ds(h0 * HD, nh * HD), pl.ds(0, nh * HD)
        stk, stv = stages[ch]
        rk, rv = rks[ch], rvs[ch]

        def put(i, carry):
            for t in range(8):
                stk[i, t, :, wide] = kag[t // 2, sqk[i, 0, t], :, cols]
                stv[i, t, :, wide] = vag[t // 2, sqv[i, 0, t], :, cols]
            return carry

        lax.fori_loop(0, 8, put, 0)

        def keep(t, carry):
            rk[xc * 8 + t] = stk[xc, t, :, wide]
            rv[zc * 8 + t] = stv[zc, t, :, wide]
            return carry

        lax.fori_loop(0, 8, keep, 0)

    def exchange(ch):
        nh = HEADS_OF[ch][1]
        wide = pl.ds(0, nh * HD)
        stk, stv = stages[ch]
        rk, rv = rks[ch], rvs[ch]
        out = []
        for i, (dx, dc) in enumerate(row_peers):
            tgt = ((x + dx) % 4) * 2 + (c + dc) % 2
            out.append(remote(stk.at[tgt, :, :, wide], rk.at[pl.ds(xc * 8, 8)], a2_s.at[ch, 0, i], a2_r.at[ch, 0, i], at(dx=dx, dc=dc)))
            tgt = ((z + dx) % 4) * 2 + (c + dc) % 2
            out.append(remote(stv.at[tgt, :, :, wide], rv.at[pl.ds(zc * 8, 8)], a2_s.at[ch, 1, i], a2_r.at[ch, 1, i], at(dz=dx, dc=dc)))
        for cp in out:
            cp.start()
        return out

    def attend(ch, lo=0, hi=16):
        h0, nh = HEADS_OF[ch]
        rk, rv = rks[ch], rvs[ch]
        lane = lax.broadcasted_iota(jnp.int32, (1, 512), 1)

        def unit(b, bias, hh):
            c0 = (h0 + hh) * HD
            cc = slice(hh * HD, (hh + 1) * HD)
            q = qv[pl.ds(pl.multiple_of(b * BLK, BLK), BLK), c0:c0 + HD]
            ks = [kx[pl.ds(b, 3), :, c0:c0 + HD].reshape(3 * BLK, HD)]
            ks += [rk[kidx[b * RANDOM + r], :, cc] for r in range(RANDOM)]
            ks += [gk[:, :, c0:c0 + HD].reshape(GLOB, HD)]
            vs = [vx[pl.ds(b, 3), :, c0:c0 + HD].reshape(3 * BLK, HD)]
            vs += [rv[vidx[b * RANDOM + r], :, cc] for r in range(RANDOM)]
            vs += [gv[:, :, c0:c0 + HD].reshape(GLOB, HD)]
            sc = lax.dot_general(q, jnp.concatenate(ks, axis=0), NT, preferred_element_type=F32)
            sc = sc + bias
            m = jnp.max(sc, axis=1, keepdims=True)
            p = jnp.exp2((sc - m) * SCALE2)
            l = jnp.sum(p, axis=1, keepdims=True)
            o = jnp.dot(p.astype(BF), jnp.concatenate(vs, axis=0), preferred_element_type=F32)
            att[pl.ds(pl.multiple_of(b * BLK, BLK), BLK), c0:c0 + HD] = (o / l).astype(BF)

        per = UNITS // nh

        def block(bb, carry):
            for k in range(per):
                b = bb * per + k
                no_left = jnp.logical_and(s == 0, b == 0)
                no_right = jnp.logical_and(s == 31, b == 15)
                low = jnp.where(no_left, BLK, 0)
                cut = jnp.where(no_right, 2 * BLK, 3 * BLK)
                gone = jnp.logical_or(lane < low, jnp.logical_and(lane >= cut, lane < 3 * BLK))
                bias = jnp.where(gone, -1e30, 0.0)
                for hh in range(nh):
                    unit(b, bias, hh)
            return carry

        lax.fori_loop(lo // per, hi // per, block, 0)

    ysends = []

    def ysend(ch):
        h0, nh = HEADS_OF[ch]
        out = []
        for h in range(h0, h0 + nh):
            for dy in (1, 3, 2):
                tgt = (y + dy) % 4
                for hf in range(2):
                    cp = remote(
                        att.at[pl.ds(tgt * 256 + hf * GLOB, GLOB), pl.ds(h * HD, HD)],
                        atts.at[h, pl.ds(hf * GLOB, GLOB), pl.ds(y * HD, HD)],
                        y_s.at[h, hf, dy], y_r.at[h, hf, dy], at(dy=dy),
                    )
                    skip = jnp.logical_and(s == 0, tgt == 0) if hf == 0 else None
                    out.append((cp, skip, root if hf == 0 else None))
        for cp, skip, _ in out:
            unless(skip, cp.start)

        def keep(hf):
            rows = pl.ds(pl.multiple_of(y * 256 + hf * GLOB, GLOB), GLOB)
            for h in range(h0, h0 + nh):
                atts[h, hf * GLOB:(hf + 1) * GLOB, pl.ds(pl.multiple_of(y * HD, HD), HD)] = att[rows, h * HD:(h + 1) * HD]

        keep(1)
        unless(root, lambda: keep(0))
        ysends.append(out)

    def yrecv(ch):
        for cp, _, skip in ysends[ch]:
            unless(skip, cp.wait_recv)

    wbufs = ((kag, 0), (vag, 0), (kag, 0), (vag, 0), (vag, 8))

    def prefetch(ch):
        h0, nh = HEADS_OF[ch]
        buf, base = wbufs[ch]
        out = []
        for h in range(nh):
            for yy in range(4):
                for n in range(4):
                    out.append(pltpu.make_async_copy(
                        wfull.at[pl.ds(yy * 16 + (h0 + h) * 2, 2), :, pl.ds(n * WIDTH, WIDTH)],
                        buf.at[n, pl.ds(base + h * 8 + yy * 2, 2)], pf.at[h0 + h, yy * 4 + n],
                    ))
        for cp in out:
            cp.start(priority=1)
        return out

    def project(ch, copies):
        h0, nh = HEADS_OF[ch]
        if ch == 3:
            nh = 2
        buf, base = wbufs[ch]
        for cp in copies:
            cp.wait()

        def tile(j, carry):
            n, sub = j // 2, j % 2
            cols = pl.ds(pl.multiple_of(j * 512, 512), 512)
            w = buf[n, base:base + nh * 8, :, pl.ds(pl.multiple_of(sub * 512, 512), 512)].reshape(nh * 512, 512)
            rows = jnp.concatenate([atts[h] for h in range(h0, h0 + nh)], axis=1)
            t = jnp.dot(rows, w, preferred_element_type=F32)
            if ch == 0:
                acc[:, cols] = t
            elif ch < 3:
                acc[:, cols] += t
            else:
                outv[:, cols] = (acc[:, cols] + t).astype(BF)
            return carry

        lax.fori_loop(0, 8, tile, 0)

    def merge(ml, part_of, n):
        m = ml(0)[0:1, :]
        for i in range(1, n):
            m = jnp.maximum(m, ml(i)[0:1, :])
        l = jnp.zeros((1, HD), F32)
        a = jnp.zeros((HD, HD), F32)
        for i in range(n):
            f = jnp.exp2((ml(i)[0:1, :] - m) * SCALE2)
            l = l + ml(i)[1:2, :] * f
            a = a + part_of(i) * f
        return m, l, a

    stage(0)
    sent = [exchange(0)]
    for cp in red1:
        cp.wait_recv()
    r1[xc] = part[xc]
    m1[xc] = pml[xc]
    m, l, a = merge(lambda i: m1[i], lambda i: r1[i].astype(F32), 8)
    comb[0:HD, :] = a
    comb[HD:HD + 8, :] = max_total(m, l)

    stage(1)
    for dz in (1, 2, 3):
        @pl.when(z == dz)
        def _(dz=dz):
            remote(comb, r2.at[dz], r2_s.at[dz], r2_r.at[dz], at(dz=4 - dz)).start()

    sent.append(exchange(1))
    stage(4)

    for cp in edges:
        cp.wait_recv()

    @pl.when(jnp.logical_and(c == 0, x != 0))
    def _():
        gcopy(gk, gk, 3, 0, at()).wait_recv()
        gcopy(gk, gk, 4, 0, mate).start()

    @pl.when(jnp.logical_and(c == 0, z != 0))
    def _():
        gcopy(gv, gv, 5, 0, at()).wait_recv()
        gcopy(gv, gv, 6, 0, mate).start()

    @pl.when(c == 1)
    def _():
        gcopy(gk, gk, 4, 0, at()).wait_recv()
        gcopy(gv, gv, 6, 0, at()).wait_recv()

    def arrived(ch):
        for cp in sent[ch]:
            cp.wait_recv()

    def refill(ch):
        for cp in sent[ch - 2]:
            cp.wait_send()
        stage(ch)
        sent.append(exchange(ch))

    agw[2].wait_recv()
    agw[3].wait_recv()
    wm += [wmate(2, left, 1), wmate(3, right, 0)]
    arrived(0)
    @pl.when(z == 0)
    def _():
        for dz in (1, 2, 3):
            remote(comb, r2.at[dz], r2_s.at[dz], r2_r.at[dz], at()).wait_recv()
        r2[0] = comb[...]
        _, l, a = merge(lambda i: r2[i, HD:HD + 8, :], lambda i: r2[i, 0:HD, :], 4)
        gout[...] = jnp.transpose(a / l).astype(BF)

    for cp in sent[0]:
        cp.wait_send()
    stage(2)
    def gfinal(yy, hh):
        return remote(gout, atts.at[hh, pl.ds(0, GLOB), pl.ds(yy * HD, HD)], r3_s, r3_r.at[yy * 8 + hh], (0, 0))

    @pl.when(z == 0)
    def _():
        @pl.when(root)
        def _():
            atts[0, 0:GLOB, 0:HD] = gout[...]

        unless(root, lambda: gfinal(y, xc).start())

    sent.append(exchange(2))
    attend(0)
    ysend(0)

    arrived(1)
    refill(3)
    sent.append(exchange(4))
    agw[4].wait_recv()
    agw[5].wait_recv()
    wm += [wmate(4, far, 0), wmate(5, far, 1)]
    attend(1)
    ysend(1)

    for g in (agk, agv):
        for cp in g:
            cp.wait_send()

    @pl.when(is00)
    def _():
        for dx in (1, 3, 2):
            gcopy(gk, gk, 3, dx, at(dx=dx)).wait_send()

    @pl.when(first)
    def _():
        for dz in (1, 3, 2):
            gcopy(gv, gv, 5, dz, at(dz=dz)).wait_send()

    @pl.when(c == 0)
    def _():
        gcopy(gk, gk, 4, 0, mate).wait_send()
        gcopy(gv, gv, 6, 0, mate).wait_send()

    wown.wait_recv()
    for cp in wm:
        cp.wait_recv()
    p0 = prefetch(0)
    p1 = prefetch(1)

    @pl.when(root)
    def _():
        for n in range(1, 32):
            gfinal(n // 8, n % 8).wait_recv()

    yrecv(0)
    project(0, p0)
    p2 = prefetch(2)
    arrived(2)
    attend(2)
    ysend(2)
    yrecv(1)
    project(1, p1)
    p3 = prefetch(3)
    p4 = prefetch(4)
    arrived(3)
    attend(3)
    ysend(3)
    arrived(4)
    attend(4)
    ysend(4)
    yrecv(2)
    project(2, p2)
    yrecv(3)
    yrecv(4)
    project(3, p3 + p4)
    done = pltpu.make_async_copy(outv, out_hbm, ob)
    done.start()

    for out in ysends:
        for cp, skip, _ in out:
            unless(skip, cp.wait_send)

    @pl.when(z == 0)
    def _():
        unless(root, lambda: gfinal(y, xc).wait_send())

    for dz in (1, 2, 3):
        @pl.when(z == dz)
        def _(dz=dz):
            remote(comb, r2.at[dz], r2_s.at[dz], r2_r.at[dz], at(dz=4 - dz)).wait_send()

    for cp in late:
        cp.wait_send()
    for cp in agw:
        cp.wait_send()
    for ch in (2, 3, 4):
        for cp in sent[ch]:
            cp.wait_send()

    @pl.when(s == 0)
    def _():
        for dz in (1, 3, 2):
            gcopy(q_top, gq, 0, dz, at(dz=dz)).wait_send()

    @pl.when(is00)
    def _():
        for dx in (1, 3, 2):
            gcopy(gq, gq, 1, dx, at(dx=dx)).wait_send()

    @pl.when(c == 0)
    def _():
        gcopy(gq, gq, 2, 0, mate).wait_send()

    done.wait()


def local(queries, key_rows, value_rows, random_owner, random_local, output_weight):
    smem = pl.BlockSpec(memory_space=pltpu.SMEM)
    hbm = pl.BlockSpec(memory_space=pl.ANY)
    dma = pltpu.SemaphoreType.DMA
    widest = max(nh for _, nh in HEADS_OF) * HD
    scratch = [
        pltpu.VMEM((4, 16, BLK, WIDTH), BF),
        pltpu.VMEM((4, 16, BLK, WIDTH), BF),
        pltpu.VMEM((18, BLK, WIDTH), BF),
        pltpu.VMEM((18, BLK, WIDTH), BF),
        pltpu.VMEM((ROWS, WIDTH), BF),
    ]
    scratch += [pltpu.VMEM((8, 8, BLK, widest), BF) for _ in range(4)]
    scratch += [pltpu.VMEM((8, 8, BLK, HEADS_OF[-1][1] * HD), BF) for _ in range(2)]
    scratch += [pltpu.VMEM((64, BLK, nh * HD), BF) for _ in range(2) for _, nh in HEADS_OF]
    scratch += [pltpu.VMEM((GLOB, WIDTH), BF)]
    scratch += [pltpu.VMEM((2, BLK, WIDTH), BF) for _ in range(2)]
    scratch += [
        pltpu.VMEM((ROWS, WIDTH), BF),
        pltpu.VMEM((8, 256, 512), BF),
        pltpu.VMEM((256, 4096), F32),
        pltpu.VMEM((256, 4096), BF),
        pltpu.VMEM((8, HD, HD), BF),
        pltpu.VMEM((8, 8, HD), F32),
        pltpu.VMEM((8, HD, HD), BF),
        pltpu.VMEM((8, 8, HD), F32),
        pltpu.VMEM((4, HD + 8, HD), F32),
        pltpu.VMEM((HD + 8, HD), F32),
        pltpu.VMEM((GLOB, HD), BF),
        pltpu.VMEM((8, 1, 128), jnp.int32),
        pltpu.VMEM((8, 1, 128), jnp.int32),
        pltpu.VMEM((8, 1, 128), jnp.int32),
        pltpu.VMEM((8, 1, 128), jnp.int32),
        pltpu.SMEM((8, 1, 128), jnp.int32),
        pltpu.SMEM((8, 1, 128), jnp.int32),
        pltpu.SMEM((16 * RANDOM,), jnp.int32),
        pltpu.SMEM((16 * RANDOM,), jnp.int32),
        dma((7,)),
        dma((2, 7)), dma((2, 7)),
        dma((2, 2)), dma((2, 2)),
        dma((2, 6)), dma((2, 6)),
        dma((1, 6)), dma((1, 6)),
        dma((7,)), dma((7,)),
        dma((CHUNKS, 2, 7)), dma((CHUNKS, 2, 7)),
        dma((7, 4)), dma((7,)),
        dma((8, 2, 4)), dma((8, 2, 4)),
        dma((2, 7)), dma((2, 7)),
        dma((4,)), dma((4,)),
        dma, dma((32,)),
        dma((8, 16)), dma,
    ]
    out, _ = pl.pallas_call(
        main_kernel,
        out_shape=[
            jax.ShapeDtypeStruct((256, 4096), BF),
            jax.ShapeDtypeStruct((64, BLK, 4096), BF),
        ],
        in_specs=[smem, smem, hbm, hbm, hbm, hbm],
        out_specs=[hbm, hbm],
        scratch_shapes=scratch,
        compiler_params=pltpu.CompilerParams(
            collective_id=0, has_side_effects=True, vmem_limit_bytes=67043328
        ),
        name="bigbird_layer",
    )(
        random_owner.T, random_local.T, queries, key_rows.reshape(16, BLK, WIDTH),
        value_rows.reshape(16, BLK, WIDTH), output_weight.reshape(16, BLK, 4096),
    )
    return out


def solution(mesh):
    return jax.shard_map(
        local,
        mesh=mesh,
        in_specs=(
            P("seq", "head"),
            P("seq", "head"),
            P("seq", "head"),
            P("seq", None),
            P("seq", None),
            P("head", None),
        ),
        out_specs=P(("seq", "head"), None),
        check_vma=False,
    )
```

```python
import math

import jax
import jax.numpy as jnp
from jax import lax
from jax.experimental import pallas as pl
from jax.experimental.pallas import tpu as pltpu
from jax.sharding import PartitionSpec as P

MESH = pl.DeviceIdType.MESH
HD = 128
BLK = 64
GLOB = 128
RANDOM = 3
UNITS = 16
ROWS = 1024
WIDTH = 1024
HEADS_OF = ((0, 2), (2, 2), (4, 2), (6, 1), (7, 1))
CHUNKS = len(HEADS_OF)
SCALE2 = HD ** (-0.5) * math.log2(math.e)
BF = jnp.bfloat16
F32 = jnp.float32
NT = (((1,), (1,)), ((), ()))
TN = (((0,), (0,)), ((), ()))


def main_kernel(
    owner, place, q_hbm, k_hbm, v_hbm, w_hbm,
    out_hbm, wfull,
    kag, vag, kx, vx, qv, stk0, stv0, stk1, stv1, stk2, stv2, *rest,
):
    rks, rvs, rest = rest[:CHUNKS], rest[CHUNKS:2 * CHUNKS], rest[2 * CHUNKS:]
    (
        gq, gk, gv, att, atts, acc, outv, part, pml, r1, m1, r2, comb, gout, reqk, reqv, rqk, rqv, sqk, sqv, kidx, vidx,
        loc, rq_s, rq_r, ed_s, ed_r, ag_s, ag_r, w_s, w_r, wd_s, wd_r,
        a2_s, a2_r, g_s, g_r, y_s, y_r, r1_s, r1_r, r2_s, r2_r, r3_s, r3_r, pf, ob,
    ) = rest
    stages = ((stk0, stv0), (stk1, stv1), (stk0, stv0), (stk1, stv1), (stk2, stv2))
    s = lax.axis_index("seq")
    y = lax.axis_index("head")
    z, x, c = s // 8, (s // 2) % 4, s % 2
    xc, zc = x * 2 + c, z * 2 + c

    def at(dz=0, dx=0, dc=0, dy=0):
        return ((((z + dz) % 4) * 4 + (x + dx) % 4) * 2 + (c + dc) % 2, (y + dy) % 4)

    def remote(src, dst, ss, rs, dev):
        return pltpu.make_async_remote_copy(
            src_ref=src, dst_ref=dst, send_sem=ss, recv_sem=rs, device_id=dev, device_id_type=MESH
        )

    def unless(cond, f):
        if cond is None:
            f()
        else:
            pl.when(jnp.logical_not(cond))(f)

    nxt, prv = ((s + 1) % 32, y), ((s + 31) % 32, y)
    row_peers = [(dx, dc) for dx in (1, 3, 2, 0) for dc in (0, 1) if (dx, dc) != (0, 0)]

    own = [
        pltpu.make_async_copy(k_hbm, kag.at[z], loc.at[0]),
        pltpu.make_async_copy(v_hbm, vag.at[x], loc.at[1]),
        pltpu.make_async_copy(k_hbm, kx.at[pl.ds(1, 16)], loc.at[2]),
        pltpu.make_async_copy(v_hbm, vx.at[pl.ds(1, 16)], loc.at[3]),
        pltpu.make_async_copy(q_hbm, qv, loc.at[4]),
    ]
    for cp in own:
        cp.start()

    bar = pltpu.get_barrier_semaphore()
    peers = [at(dx=dx, dc=dc) for dx, dc in row_peers]
    peers += [at(dz=dz, dc=dc) for dz in (1, 2, 3) for dc in (0, 1)]
    peers += [at(dy=dy) for dy in (1, 2, 3)]
    peers += [nxt, prv]
    for dev in peers:
        pl.semaphore_signal(bar, inc=1, device_id=dev, device_id_type=MESH)
    root = jnp.logical_and(s == 0, y == 0)

    @pl.when(z == 0)
    def _():
        @pl.when(jnp.logical_not(root))
        def _():
            pl.semaphore_signal(bar, inc=1, device_id=(0, 0), device_id_type=MESH)

    @pl.when(root)
    def _():
        for ss in range(8):
            for yy in range(4):
                if (ss, yy) != (0, 0):
                    pl.semaphore_signal(bar, inc=1, device_id=(ss, yy), device_id_type=MESH)
        pl.semaphore_wait(bar, len(peers) + 31)

    @pl.when(jnp.logical_not(root))
    def _():
        @pl.when(z == 0)
        def _():
            pl.semaphore_wait(bar, len(peers) + 1)

        @pl.when(z != 0)
        def _():
            pl.semaphore_wait(bar, len(peers))

    late = []

    def go(cp):
        cp.start()
        late.append(cp)
        return cp

    is00 = jnp.logical_and(x == 0, c == 0)
    mate = at(dc=1)

    def gcopy(src, dst, n, i, dev):
        return remote(src, dst, g_s.at[n, i], g_r.at[n], dev)

    q_top = q_hbm.at[pl.ds(0, GLOB)]
    q_root = pltpu.make_async_copy(q_top, gq, g_r.at[0])

    @pl.when(s == 0)
    def _():
        q_root.start()
        for dz in (1, 3, 2):
            gcopy(q_top, gq, 0, dz, at(dz=dz)).start()

    def gather(n, own_view, view, up, down, me, ss, rs):
        a = remote(own_view(0), view(me, 0), ss.at[n, 0], rs.at[n, 0], up)
        b = remote(own_view(1), view(me, 1), ss.at[n, 1], rs.at[n, 1], down)
        d = remote(own_view(1), view(me, 1), ss.at[n, 2], rs.at[n, 2], up)
        e = remote(own_view(0), view(me, 0), ss.at[n, 3], rs.at[n, 3], down)
        before, after = (me + 3) % 4, (me + 1) % 4
        f = remote(view(before, 0), view(before, 0), ss.at[n, 4], rs.at[n, 4], up)
        g = remote(view(after, 1), view(after, 1), ss.at[n, 5], rs.at[n, 5], down)
        return a, b, d, e, f, g

    agk = gather(
        0, lambda p: k_hbm.at[pl.ds(p * 8, 8)],
        lambda m, p: kag.at[m, pl.ds(p * 8, 8)], at(dz=1), at(dz=3), z, ag_s, ag_r,
    )
    agv = gather(
        1, lambda p: v_hbm.at[pl.ds(p * 8, 8)],
        lambda m, p: vag.at[m, pl.ds(p * 8, 8)], at(dx=1), at(dx=3), x, ag_s, ag_r,
    )

    def wview(m, p):
        return wfull.at[pl.ds(m * 16 + c * 8 + p * 4, 4)]

    agw = gather(
        0, lambda p: w_hbm.at[pl.ds(c * 8 + p * 4, 4)],
        wview, at(dy=1), at(dy=3), y, w_s, w_r,
    )
    for n in range(4):
        for g in (agk, agv, agw):
            g[n].start()

    edges = []
    for i, (hbm, ext) in enumerate(((k_hbm, kx), (v_hbm, vx))):
        edges.append(go(remote(hbm.at[0], ext.at[17], ed_s.at[i, 0], ed_r.at[i, 0], prv)))
        edges.append(go(remote(hbm.at[15], ext.at[0], ed_s.at[i, 1], ed_r.at[i, 1], nxt)))

    wown = go(remote(w_hbm, wfull.at[pl.ds(y * 16, 16)], wd_s.at[6], wd_r.at[6], mate))

    @pl.when(is00)
    def _():
        @pl.when(s == 0)
        def _():
            q_root.wait()

        @pl.when(s != 0)
        def _():
            gcopy(q_top, gq, 0, 0, at()).wait_recv()

        for dx in (1, 3, 2):
            gcopy(gq, gq, 1, dx, at(dx=dx)).start()

    reqk[...] = jnp.zeros((8, 1, 128), jnp.int32)
    reqv[...] = jnp.zeros((8, 1, 128), jnp.int32)
    lanes = lax.broadcasted_iota(jnp.int32, (1, 128), 1)

    def serve(o, carry):
        def look(b, st):
            n, p0, p1 = st
            for r in range(RANDOM):
                hit = owner[r, b] == o
                here = place[r, b]
                p0 = jnp.where(jnp.logical_and(hit, n == 0), here, p0)
                p1 = jnp.where(jnp.logical_and(hit, n == 1), here, p1)
                n = n + jnp.where(hit, 1, 0)
            return n, p0, p1

        zero = jnp.int32(0)
        _, p0, p1 = lax.fori_loop(0, 16, look, (zero, zero, zero))
        oz, ox, oc = o // 8, (o // 2) % 4, o % 2

        def row(old, t):
            return jnp.where(lanes == t, p0, jnp.where(lanes == t + 1, p1, old))

        reqk[ox * 2 + oc] = row(reqk[ox * 2 + oc], oz * 2)
        reqv[oz * 2 + oc] = row(reqv[oz * 2 + oc], ox * 2)
        return carry

    lax.fori_loop(0, 32, serve, 0)

    def number(b, carry):
        for r in range(RANDOM):
            o = owner[r, b]

            def before(bb, n):
                for rr in range(RANDOM):
                    n = n + jnp.where(owner[rr, bb] == o, 1, 0)
                return n

            n = lax.fori_loop(0, b, before, jnp.int32(0))
            oz, ox, oc = o // 8, (o // 2) % 4, o % 2
            kidx[b * RANDOM + r] = (ox * 2 + oc) * 8 + oz * 2 + n
            vidx[b * RANDOM + r] = (oz * 2 + oc) * 8 + ox * 2 + n
        return carry

    lax.fori_loop(0, 16, number, 0)

    rq = []
    for i, (dx, dc) in enumerate(row_peers):
        tgt = ((x + dx) % 4) * 2 + (c + dc) % 2
        rq.append(go(remote(reqk.at[tgt], rqk.at[xc], rq_s.at[0, i], rq_r.at[0, i], at(dx=dx, dc=dc))))
        tgt = ((z + dx) % 4) * 2 + (c + dc) % 2
        rq.append(go(remote(reqv.at[tgt], rqv.at[zc], rq_s.at[1, i], rq_r.at[1, i], at(dz=dx, dc=dc))))

    def forward(g):
        g[0].wait_recv()
        g[4].start()
        g[1].wait_recv()
        g[5].start()

    forward(agk)
    forward(agv)
    for cp in own:
        cp.wait()

    @pl.when(c == 0)
    def _():
        @pl.when(x != 0)
        def _():
            gcopy(gq, gq, 1, 0, at()).wait_recv()

        gcopy(gq, gq, 2, 0, mate).start()

    @pl.when(c == 1)
    def _():
        gcopy(gq, gq, 2, 0, at()).wait_recv()

    left, right, far = (y + 3) % 4, (y + 1) % 4, (y + 2) % 4

    def wmate(n, m, p):
        return go(remote(wview(m, p), wview(m, p), wd_s.at[n], wd_r.at[n], mate))

    row8 = lax.broadcasted_iota(jnp.int32, (8, HD), 0)

    def max_total(m, l):
        return jnp.where(row8 == 0, m, jnp.where(row8 == 1, l, 0.0))

    def glob(h, carry):
        cols = pl.ds(pl.multiple_of(h * HD, HD), HD)
        kk = kx[1:17, :, cols].reshape(ROWS, HD)
        vv = vx[1:17, :, cols].reshape(ROWS, HD)
        st = lax.dot_general(kk, gq[:, cols], NT, preferred_element_type=F32)
        m = jnp.max(st, axis=0, keepdims=True)
        p = jnp.exp2((st - m) * SCALE2)
        l = jnp.sum(p, axis=0, keepdims=True)
        part[h] = lax.dot_general(vv, p.astype(BF), TN, preferred_element_type=F32).astype(BF)
        pml[h] = max_total(m, l)
        return carry

    lax.fori_loop(0, 8, glob, 0)

    forward(agw)
    wm = [wmate(0, left, 0), wmate(1, right, 1)]

    red1 = []
    for i, (dx, dc) in enumerate(row_peers):
        tgt = ((x + dx) % 4) * 2 + (c + dc) % 2
        red1.append(go(remote(part.at[tgt], r1.at[xc], r1_s.at[0, i], r1_r.at[0, i], at(dx=dx, dc=dc))))
        red1.append(go(remote(pml.at[tgt], m1.at[xc], r1_s.at[1, i], r1_r.at[1, i], at(dx=dx, dc=dc))))

    for cp in rq:
        cp.wait_recv()
    rqk[xc] = reqk[xc]
    rqv[zc] = reqv[zc]
    to_s = [pltpu.make_async_copy(rqk, sqk, loc.at[5]), pltpu.make_async_copy(rqv, sqv, loc.at[6])]
    for cp in to_s:
        cp.start()
    for cp in to_s:
        cp.wait()

    for g in (agk, agv):
        for cp in g[2:]:
            cp.wait_recv()

    @pl.when(is00)
    def _():
        for dx in (1, 3, 2):
            gcopy(kag.at[0, pl.ds(0, 2)], gk, 3, dx, at(dx=dx)).start()
        gcopy(kag.at[0, pl.ds(0, 2)], gk, 4, 0, mate).start()
        gk[...] = kag[0, 0:2]

    first = jnp.logical_and(z == 0, c == 0)

    @pl.when(first)
    def _():
        for dz in (1, 3, 2):
            gcopy(vag.at[0, pl.ds(0, 2)], gv, 5, dz, at(dz=dz)).start()
        gcopy(vag.at[0, pl.ds(0, 2)], gv, 6, 0, mate).start()
        gv[...] = vag[0, 0:2]

    def stage(ch):
        h0, nh = HEADS_OF[ch]
        cols, wide = pl.ds(h0 * HD, nh * HD), pl.ds(0, nh * HD)
        stk, stv = stages[ch]
        rk, rv = rks[ch], rvs[ch]

        def put(i, carry):
            for t in range(8):
                stk[i, t, :, wide] = kag[t // 2, sqk[i, 0, t], :, cols]
                stv[i, t, :, wide] = vag[t // 2, sqv[i, 0, t], :, cols]
            return carry

        lax.fori_loop(0, 8, put, 0)

        def keep(t, carry):
            rk[xc * 8 + t] = stk[xc, t, :, wide]
            rv[zc * 8 + t] = stv[zc, t, :, wide]
            return carry

        lax.fori_loop(0, 8, keep, 0)

    def exchange(ch):
        nh = HEADS_OF[ch][1]
        wide = pl.ds(0, nh * HD)
        stk, stv = stages[ch]
        rk, rv = rks[ch], rvs[ch]
        out = []
        for i, (dx, dc) in enumerate(row_peers):
            tgt = ((x + dx) % 4) * 2 + (c + dc) % 2
            out.append(remote(stk.at[tgt, :, :, wide], rk.at[pl.ds(xc * 8, 8)], a2_s.at[ch, 0, i], a2_r.at[ch, 0, i], at(dx=dx, dc=dc)))
            tgt = ((z + dx) % 4) * 2 + (c + dc) % 2
            out.append(remote(stv.at[tgt, :, :, wide], rv.at[pl.ds(zc * 8, 8)], a2_s.at[ch, 1, i], a2_r.at[ch, 1, i], at(dz=dx, dc=dc)))
        for cp in out:
            cp.start()
        return out

    def attend(ch, lo=0, hi=16):
        h0, nh = HEADS_OF[ch]
        rk, rv = rks[ch], rvs[ch]
        lane = lax.broadcasted_iota(jnp.int32, (1, 512), 1)

        def unit(b, bias, hh):
            c0 = (h0 + hh) * HD
            cc = slice(hh * HD, (hh + 1) * HD)
            q = qv[pl.ds(pl.multiple_of(b * BLK, BLK), BLK), c0:c0 + HD]
            ks = [kx[pl.ds(b, 3), :, c0:c0 + HD].reshape(3 * BLK, HD)]
            ks += [rk[kidx[b * RANDOM + r], :, cc] for r in range(RANDOM)]
            ks += [gk[:, :, c0:c0 + HD].reshape(GLOB, HD)]
            vs = [vx[pl.ds(b, 3), :, c0:c0 + HD].reshape(3 * BLK, HD)]
            vs += [rv[vidx[b * RANDOM + r], :, cc] for r in range(RANDOM)]
            vs += [gv[:, :, c0:c0 + HD].reshape(GLOB, HD)]
            sc = lax.dot_general(q, jnp.concatenate(ks, axis=0), NT, preferred_element_type=F32)
            sc = sc + bias
            m = jnp.max(sc, axis=1, keepdims=True)
            p = jnp.exp2((sc - m) * SCALE2)
            l = jnp.sum(p, axis=1, keepdims=True)
            o = jnp.dot(p.astype(BF), jnp.concatenate(vs, axis=0), preferred_element_type=F32)
            att[pl.ds(pl.multiple_of(b * BLK, BLK), BLK), c0:c0 + HD] = (o / l).astype(BF)

        per = UNITS // nh

        def block(bb, carry):
            for k in range(per):
                b = bb * per + k
                no_left = jnp.logical_and(s == 0, b == 0)
                no_right = jnp.logical_and(s == 31, b == 15)
                low = jnp.where(no_left, BLK, 0)
                cut = jnp.where(no_right, 2 * BLK, 3 * BLK)
                gone = jnp.logical_or(lane < low, jnp.logical_and(lane >= cut, lane < 3 * BLK))
                bias = jnp.where(gone, -1e30, 0.0)
                for hh in range(nh):
                    unit(b, bias, hh)
            return carry

        lax.fori_loop(lo // per, hi // per, block, 0)

    ysends = []

    def ysend(ch):
        h0, nh = HEADS_OF[ch]
        out = []
        for h in range(h0, h0 + nh):
            for dy in (1, 3, 2):
                tgt = (y + dy) % 4
                for hf in range(2):
                    cp = remote(
                        att.at[pl.ds(tgt * 256 + hf * GLOB, GLOB), pl.ds(h * HD, HD)],
                        atts.at[h, pl.ds(hf * GLOB, GLOB), pl.ds(y * HD, HD)],
                        y_s.at[h, hf, dy], y_r.at[h, hf, dy], at(dy=dy),
                    )
                    skip = jnp.logical_and(s == 0, tgt == 0) if hf == 0 else None
                    out.append((cp, skip, root if hf == 0 else None))
        for cp, skip, _ in out:
            unless(skip, cp.start)

        def keep(hf):
            rows = pl.ds(pl.multiple_of(y * 256 + hf * GLOB, GLOB), GLOB)
            for h in range(h0, h0 + nh):
                atts[h, hf * GLOB:(hf + 1) * GLOB, pl.ds(pl.multiple_of(y * HD, HD), HD)] = att[rows, h * HD:(h + 1) * HD]

        keep(1)
        unless(root, lambda: keep(0))
        ysends.append(out)

    def yrecv(ch):
        for cp, _, skip in ysends[ch]:
            unless(skip, cp.wait_recv)

    wbufs = ((kag, 0), (vag, 0), (kag, 0), (vag, 0), (vag, 8))

    def prefetch(ch):
        h0, nh = HEADS_OF[ch]
        buf, base = wbufs[ch]
        out = []
        for h in range(nh):
            for yy in range(4):
                for n in range(4):
                    out.append(pltpu.make_async_copy(
                        wfull.at[pl.ds(yy * 16 + (h0 + h) * 2, 2), :, pl.ds(n * WIDTH, WIDTH)],
                        buf.at[n, pl.ds(base + h * 8 + yy * 2, 2)], pf.at[h0 + h, yy * 4 + n],
                    ))
        for cp in out:
            cp.start(priority=1)
        return out

    def project(ch, copies):
        h0, nh = HEADS_OF[ch]
        if ch == 3:
            nh = 2
        buf, base = wbufs[ch]
        for cp in copies:
            cp.wait()

        def tile(j, carry):
            n, sub = j // 2, j % 2
            cols = pl.ds(pl.multiple_of(j * 512, 512), 512)
            w = buf[n, base:base + nh * 8, :, pl.ds(pl.multiple_of(sub * 512, 512), 512)].reshape(nh * 512, 512)
            rows = jnp.concatenate([atts[h] for h in range(h0, h0 + nh)], axis=1)
            t = jnp.dot(rows, w, preferred_element_type=F32)
            if ch == 0:
                acc[:, cols] = t
            elif ch < 3:
                acc[:, cols] += t
            else:
                outv[:, cols] = (acc[:, cols] + t).astype(BF)

                @pl.when(jnp.logical_and(j % 2 == 0, j > 0))
                def _():
                    wide = pl.ds(pl.multiple_of((n - 1) * WIDTH, WIDTH), WIDTH)
                    pltpu.make_async_copy(outv.at[:, wide], out_hbm.at[:, wide], ob.at[n - 1]).start()
            return carry

        lax.fori_loop(0, 8, tile, 0)

    def merge(ml, part_of, n):
        m = ml(0)[0:1, :]
        for i in range(1, n):
            m = jnp.maximum(m, ml(i)[0:1, :])
        l = jnp.zeros((1, HD), F32)
        a = jnp.zeros((HD, HD), F32)
        for i in range(n):
            f = jnp.exp2((ml(i)[0:1, :] - m) * SCALE2)
            l = l + ml(i)[1:2, :] * f
            a = a + part_of(i) * f
        return m, l, a

    stage(0)
    sent = [exchange(0)]
    for cp in red1:
        cp.wait_recv()
    r1[xc] = part[xc]
    m1[xc] = pml[xc]
    m, l, a = merge(lambda i: m1[i], lambda i: r1[i].astype(F32), 8)
    comb[0:HD, :] = a
    comb[HD:HD + 8, :] = max_total(m, l)

    stage(1)
    for dz in (1, 2, 3):
        @pl.when(z == dz)
        def _(dz=dz):
            remote(comb, r2.at[dz], r2_s.at[dz], r2_r.at[dz], at(dz=4 - dz)).start()

    sent.append(exchange(1))
    stage(4)

    for cp in edges:
        cp.wait_recv()

    @pl.when(jnp.logical_and(c == 0, x != 0))
    def _():
        gcopy(gk, gk, 3, 0, at()).wait_recv()
        gcopy(gk, gk, 4, 0, mate).start()

    @pl.when(jnp.logical_and(c == 0, z != 0))
    def _():
        gcopy(gv, gv, 5, 0, at()).wait_recv()
        gcopy(gv, gv, 6, 0, mate).start()

    @pl.when(c == 1)
    def _():
        gcopy(gk, gk, 4, 0, at()).wait_recv()
        gcopy(gv, gv, 6, 0, at()).wait_recv()

    def arrived(ch):
        for cp in sent[ch]:
            cp.wait_recv()

    def refill(ch):
        for cp in sent[ch - 2]:
            cp.wait_send()
        stage(ch)
        sent.append(exchange(ch))

    agw[2].wait_recv()
    agw[3].wait_recv()
    wm += [wmate(2, left, 1), wmate(3, right, 0)]
    arrived(0)
    @pl.when(z == 0)
    def _():
        for dz in (1, 2, 3):
            remote(comb, r2.at[dz], r2_s.at[dz], r2_r.at[dz], at()).wait_recv()
        r2[0] = comb[...]
        _, l, a = merge(lambda i: r2[i, HD:HD + 8, :], lambda i: r2[i, 0:HD, :], 4)
        gout[...] = jnp.transpose(a / l).astype(BF)

    for cp in sent[0]:
        cp.wait_send()
    stage(2)
    def gfinal(yy, hh):
        return remote(gout, atts.at[hh, pl.ds(0, GLOB), pl.ds(yy * HD, HD)], r3_s, r3_r.at[yy * 8 + hh], (0, 0))

    @pl.when(z == 0)
    def _():
        @pl.when(root)
        def _():
            atts[0, 0:GLOB, 0:HD] = gout[...]

        unless(root, lambda: gfinal(y, xc).start())

    sent.append(exchange(2))
    attend(0)
    ysend(0)

    arrived(1)
    refill(3)
    sent.append(exchange(4))
    agw[4].wait_recv()
    agw[5].wait_recv()
    wm += [wmate(4, far, 0), wmate(5, far, 1)]
    attend(1)
    ysend(1)

    for g in (agk, agv):
        for cp in g:
            cp.wait_send()

    @pl.when(is00)
    def _():
        for dx in (1, 3, 2):
            gcopy(gk, gk, 3, dx, at(dx=dx)).wait_send()

    @pl.when(first)
    def _():
        for dz in (1, 3, 2):
            gcopy(gv, gv, 5, dz, at(dz=dz)).wait_send()

    @pl.when(c == 0)
    def _():
        gcopy(gk, gk, 4, 0, mate).wait_send()
        gcopy(gv, gv, 6, 0, mate).wait_send()

    wown.wait_recv()
    for cp in wm:
        cp.wait_recv()
    p0 = prefetch(0)
    p1 = prefetch(1)

    @pl.when(root)
    def _():
        for n in range(1, 32):
            gfinal(n // 8, n % 8).wait_recv()

    yrecv(0)
    project(0, p0)
    p2 = prefetch(2)
    arrived(2)
    attend(2)
    ysend(2)
    yrecv(1)
    project(1, p1)
    p3 = prefetch(3)
    p4 = prefetch(4)
    arrived(3)
    attend(3)
    ysend(3)
    arrived(4)
    attend(4)
    ysend(4)
    yrecv(2)
    project(2, p2)
    yrecv(3)
    yrecv(4)
    project(3, p3 + p4)

    last = pl.ds(3 * WIDTH, WIDTH)
    pltpu.make_async_copy(outv.at[:, last], out_hbm.at[:, last], ob.at[3]).start()

    for out in ysends:
        for cp, skip, _ in out:
            unless(skip, cp.wait_send)

    @pl.when(z == 0)
    def _():
        unless(root, lambda: gfinal(y, xc).wait_send())

    for dz in (1, 2, 3):
        @pl.when(z == dz)
        def _(dz=dz):
            remote(comb, r2.at[dz], r2_s.at[dz], r2_r.at[dz], at(dz=4 - dz)).wait_send()

    for cp in late:
        cp.wait_send()
    for cp in agw:
        cp.wait_send()
    for ch in (2, 3, 4):
        for cp in sent[ch]:
            cp.wait_send()

    @pl.when(s == 0)
    def _():
        for dz in (1, 3, 2):
            gcopy(q_top, gq, 0, dz, at(dz=dz)).wait_send()

    @pl.when(is00)
    def _():
        for dx in (1, 3, 2):
            gcopy(gq, gq, 1, dx, at(dx=dx)).wait_send()

    @pl.when(c == 0)
    def _():
        gcopy(gq, gq, 2, 0, mate).wait_send()

    for n in range(4):
        wide = pl.ds(n * WIDTH, WIDTH)
        pltpu.make_async_copy(outv.at[:, wide], out_hbm.at[:, wide], ob.at[n]).wait()


def local(queries, key_rows, value_rows, random_owner, random_local, output_weight):
    smem = pl.BlockSpec(memory_space=pltpu.SMEM)
    hbm = pl.BlockSpec(memory_space=pl.ANY)
    dma = pltpu.SemaphoreType.DMA
    widest = max(nh for _, nh in HEADS_OF) * HD
    scratch = [
        pltpu.VMEM((4, 16, BLK, WIDTH), BF),
        pltpu.VMEM((4, 16, BLK, WIDTH), BF),
        pltpu.VMEM((18, BLK, WIDTH), BF),
        pltpu.VMEM((18, BLK, WIDTH), BF),
        pltpu.VMEM((ROWS, WIDTH), BF),
    ]
    scratch += [pltpu.VMEM((8, 8, BLK, widest), BF) for _ in range(4)]
    scratch += [pltpu.VMEM((8, 8, BLK, HEADS_OF[-1][1] * HD), BF) for _ in range(2)]
    scratch += [pltpu.VMEM((64, BLK, nh * HD), BF) for _ in range(2) for _, nh in HEADS_OF]
    scratch += [pltpu.VMEM((GLOB, WIDTH), BF)]
    scratch += [pltpu.VMEM((2, BLK, WIDTH), BF) for _ in range(2)]
    scratch += [
        pltpu.VMEM((ROWS, WIDTH), BF),
        pltpu.VMEM((8, 256, 512), BF),
        pltpu.VMEM((256, 4096), F32),
        pltpu.VMEM((256, 4096), BF),
        pltpu.VMEM((8, HD, HD), BF),
        pltpu.VMEM((8, 8, HD), F32),
        pltpu.VMEM((8, HD, HD), BF),
        pltpu.VMEM((8, 8, HD), F32),
        pltpu.VMEM((4, HD + 8, HD), F32),
        pltpu.VMEM((HD + 8, HD), F32),
        pltpu.VMEM((GLOB, HD), BF),
        pltpu.VMEM((8, 1, 128), jnp.int32),
        pltpu.VMEM((8, 1, 128), jnp.int32),
        pltpu.VMEM((8, 1, 128), jnp.int32),
        pltpu.VMEM((8, 1, 128), jnp.int32),
        pltpu.SMEM((8, 1, 128), jnp.int32),
        pltpu.SMEM((8, 1, 128), jnp.int32),
        pltpu.SMEM((16 * RANDOM,), jnp.int32),
        pltpu.SMEM((16 * RANDOM,), jnp.int32),
        dma((7,)),
        dma((2, 7)), dma((2, 7)),
        dma((2, 2)), dma((2, 2)),
        dma((2, 6)), dma((2, 6)),
        dma((1, 6)), dma((1, 6)),
        dma((7,)), dma((7,)),
        dma((CHUNKS, 2, 7)), dma((CHUNKS, 2, 7)),
        dma((7, 4)), dma((7,)),
        dma((8, 2, 4)), dma((8, 2, 4)),
        dma((2, 7)), dma((2, 7)),
        dma((4,)), dma((4,)),
        dma, dma((32,)),
        dma((8, 16)), dma((4,)),
    ]
    out, _ = pl.pallas_call(
        main_kernel,
        out_shape=[
            jax.ShapeDtypeStruct((256, 4096), BF),
            jax.ShapeDtypeStruct((64, BLK, 4096), BF),
        ],
        in_specs=[smem, smem, hbm, hbm, hbm, hbm],
        out_specs=[hbm, hbm],
        scratch_shapes=scratch,
        compiler_params=pltpu.CompilerParams(
            collective_id=0, has_side_effects=True, vmem_limit_bytes=67043328
        ),
        name="bigbird_layer",
    )(
        random_owner.T, random_local.T, queries, key_rows.reshape(16, BLK, WIDTH),
        value_rows.reshape(16, BLK, WIDTH), output_weight.reshape(16, BLK, 4096),
    )
    return out


def solution(mesh):
    return jax.shard_map(
        local,
        mesh=mesh,
        in_specs=(
            P("seq", "head"),
            P("seq", "head"),
            P("seq", "head"),
            P("seq", None),
            P("seq", None),
            P("head", None),
        ),
        out_specs=P(("seq", "head"), None),
        check_vma=False,
    )
```
